32 devices in a mesh: dp: 8 (over z, y), tensor: 4 (over x, core).
Axes of the slice: x: 2, y: 2, z: 4, core: 2. Of those that a mesh axis runs over, the one named last changes fastest.
Arguments:
- layer_outs: bfloat16 [5, 8192, 4096], P(None, 'dp', 'tensor'), may hold values from -6 to 6
- avg_grads: bfloat16 [4, 8192, 4096], P(None, 'dp', 'tensor'), may hold values from -0.0010299683 to 0.0010299683
- attn_mixed: bfloat16 [8192, 4096], P('dp', 'tensor'), may hold values from -96 to 96
- dwa_coefs: float32 [4, 5], replicated, may hold values from -1.5 to 1.5
Outputs:
- coef_grad: float32 [4, 5], replicated
- proj_grad: float32 [4096, 4096], P('dp', 'tensor')
The draws below stay inside these ranges and needn't reach their ends.
All inputs are finite; a program needn't handle non-finite values.
Results may differ from the reference program's by a relative error of at most 0.0042.
Values may be sent and summed in bfloat16 or wider, within the bound.
A program may use at most 128 MiB of HBM per device.

```python
import jax
import jax.numpy as jnp
from jax import lax

D = 4096
LAYERS = 4
TOKENS = 8192


def steps_of(rng, dims, split, least, largest):
    factor_of, own = 1.0, jax.random.fold_in(rng, 6)
    for dim, blocks in split:
        heights = jnp.exp(jax.random.uniform(jax.random.fold_in(own, dim), (blocks,), jnp.float32, least / len(split), largest / len(split)))
        factor_of = factor_of * jnp.repeat(heights, dims[dim] // blocks).reshape([-1 if axis == dim else 1 for axis in range(len(dims))])
    return factor_of


def bell_draw(own_key, dims, scale, bound, split=(), kind=jnp.bfloat16):
    array = scale * jax.random.normal(own_key, dims, jnp.float32)
    if split:
        array = array * steps_of(own_key, dims, split, -0.22, 0.18)
    return jnp.clip(array, -bound, bound).astype(kind)


def setup_inputs(seed: int = 0) -> dict:
    keys = jax.random.split(jax.random.key(seed), 5)
    layer_outs = bell_draw(keys[0], (LAYERS + 1, TOKENS, D), 1.0, 6.0, ((1, 8), (2, 4)))
    avg_grads = bell_draw(keys[1], (LAYERS, TOKENS, D), (1.0 / (TOKENS * D) ** 0.5), 0.0010299683, ((1, 8), (2, 4)))
    attn_mixed = bell_draw(keys[2], (TOKENS, D), (D ** 0.5 / 4), 96.0, ((0, 8), (1, 4)))
    dwa_coefs = jnp.clip(jax.random.uniform(keys[3], (LAYERS, LAYERS + 1), jnp.float32, -1.5, 1.5), -1.5, 1.5)
    return dict(layer_outs=layer_outs, avg_grads=avg_grads, attn_mixed=attn_mixed, dwa_coefs=dwa_coefs)


def reference(layer_outs, avg_grads, attn_mixed, dwa_coefs):
    grads_flat = avg_grads.reshape(LAYERS, -1)
    outs_flat = layer_outs.reshape(LAYERS + 1, -1)
    raw = lax.dot_general(grads_flat, outs_flat, (((1,), (1,)), ((), ())), preferred_element_type=jnp.float32)
    rows = jnp.arange(LAYERS, dtype=jnp.int32)[:, None]
    cols = jnp.arange(LAYERS + 1, dtype=jnp.int32)[None, :]
    coef_grad = jnp.where(cols <= rows + 1, raw, jnp.float32(0.0))
    first = dwa_coefs[LAYERS - 2, LAYERS - 1] * avg_grads[LAYERS - 2].astype(jnp.float32)
    second = dwa_coefs[LAYERS - 1, LAYERS - 1] * avg_grads[LAYERS - 1].astype(jnp.float32)
    out_grad = (first + second).astype(jnp.bfloat16)
    proj_grad = lax.dot_general(out_grad, attn_mixed, (((0,), (0,)), ((), ())), preferred_element_type=jnp.float32)
    return coef_grad, proj_grad
```

```python
import functools

import jax
import jax.numpy as jnp
from jax import lax
from jax.experimental import pallas as pl
from jax.experimental.pallas import tpu as pltpu
from jax.sharding import PartitionSpec as P

LANES = 128
LAG = 3
SKEW = 2


def kernel(
    dp_size, tensor_size, outs_hbm, grads_hbm, attn_hbm, coefs, coef_out, proj_out,
    outs, grads, attn, gathered, g_send, own, z_send, z_left, z_right, sums_ref, coef_a, coef_b, coef_c,
    load_sem, attn_sem, gy_sem, p_sem, x_sem, g_recv, a_sem, a_recv,
    z_send_sem, zl_sem, zr_sem, ca_send, ca_recv, cb_send, cb_recv,
):
    depth, tokens, features = grads.shape
    rows, cols = proj_out.shape
    strips = cols // LANES
    chunks = rows // LANES
    early = max(chunks // 2, 1)
    ys = dp_size // tensor_size
    zs = tensor_size
    xs = tensor_size // 2
    dp, tensor = lax.axis_index("dp"), lax.axis_index("tensor")
    z, y = dp // ys, dp % ys
    x, core = tensor // 2, tensor % 2
    partner = x * 2 + 1 - core
    beside = jnp.where(z == 0, 1, jnp.where(z == zs - 1, zs - 2, -1))
    two = min(2, strips)
    mesh_id = pl.DeviceIdType.MESH

    loads = []
    for i in (depth - 2, depth - 1):
        loads.append(pltpu.make_async_copy(grads_hbm.at[i], grads.at[i], load_sem.at[i]))
    for i in range(depth - 2):
        loads.append(pltpu.make_async_copy(grads_hbm.at[i], grads.at[i], load_sem.at[i]))
    for j in range(depth + 1):
        loads.append(pltpu.make_async_copy(outs_hbm.at[j], outs.at[j], load_sem.at[depth + j]))
    mine = pl.ds(pl.multiple_of(y * tokens, tokens), tokens)
    attn_loads = [
        pltpu.make_async_copy(
            attn_hbm.at[:, pl.ds(k * LANES, LANES)], attn.at[k, mine, :], attn_sem.at[k]
        )
        for k in range(strips)
    ]
    loads[0].start()
    loads[1].start()
    for load in attn_loads:
        load.start()
    for load in loads[2:]:
        load.start()

    barrier = pltpu.get_barrier_semaphore()

    def greet(**device):
        pl.semaphore_signal(barrier, inc=1, device_id=device, device_id_type=mesh_id)

    greet(tensor=partner)
    for i in range(1, ys):
        greet(dp=z * ys + (y + i) % ys)
    for n in range(1, xs):
        greet(tensor=(x + n) % xs * 2 + core)

    @pl.when(z > 0)
    def _():
        greet(dp=dp - ys)

    @pl.when(z < zs - 1)
    def _():
        greet(dp=dp + ys)

    def meet():
        ends = jnp.where(z == 0, 1, 0) + jnp.where(z == zs - 1, 1, 0)
        pl.semaphore_wait(barrier, 1 + (ys - 1) + (xs - 1) + 2 - ends)

    def lane_rows(c, count=1):
        return pl.ds(c * LANES, LANES * count)

    def piece(slot, part, c):
        return gathered.at[slot, part, lane_rows(c), :]

    def y_copy(i, c):
        return pltpu.make_async_remote_copy(
            src_ref=g_send.at[i - 1, lane_rows(c), :], dst_ref=piece(tensor, y, c),
            send_sem=gy_sem.at[i - 1, c], recv_sem=g_recv.at[tensor, y, c],
            device_id={"dp": z * ys + (y + i) % ys}, device_id_type=mesh_id,
        )

    def partner_copy(slot, part, c):
        return pltpu.make_async_remote_copy(
            src_ref=piece(slot, part, c), dst_ref=piece(slot, part, c),
            send_sem=p_sem.at[slot // 2, part, c], recv_sem=g_recv.at[slot, part, c],
            device_id={"tensor": partner}, device_id_type=mesh_id,
        )

    def x_copy(n, part, c):
        return pltpu.make_async_remote_copy(
            src_ref=piece(tensor, part, c), dst_ref=piece(tensor, part, c),
            send_sem=x_sem.at[n - 1, part, c], recv_sem=g_recv.at[tensor, part, c],
            device_id={"tensor": (x + n) % xs * 2 + core}, device_id_type=mesh_id,
        )

    def arrive(slot, part, c):
        partner_copy(slot, part, c).wait_recv()

    def attn_copy(i, k):
        return pltpu.make_async_remote_copy(
            src_ref=attn.at[k, mine, :], dst_ref=attn.at[k, mine, :],
            send_sem=a_sem.at[i - 1, k], recv_sem=a_recv.at[y, k],
            device_id={"dp": z * ys + (y + i) % ys}, device_id_type=mesh_id,
        )

    def attn_arrive(k):
        for i in range(1, ys):
            part = (y + i) % ys
            there = pl.ds(pl.multiple_of(part * tokens, tokens), tokens)
            pltpu.make_async_remote_copy(
                src_ref=attn.at[k, there, :], dst_ref=attn.at[k, there, :],
                send_sem=a_sem.at[i - 1, k], recv_sem=a_recv.at[part, k],
                device_id={"dp": z * ys + part}, device_id_type=mesh_id,
            ).wait_recv()

    def make(part, c, into):
        first, second = coefs[depth - 2, depth - 1], coefs[depth - 1, depth - 1]

        @pl.loop(0, tokens // LANES)
        def _(step):
            at = pl.ds(pl.multiple_of(step * LANES, LANES), LANES)
            wide = pl.ds(pl.multiple_of(part * rows + c * LANES, LANES), LANES)
            value = first * grads[depth - 2, at, wide].astype(jnp.float32)
            value += second * grads[depth - 1, at, wide].astype(jnp.float32)
            into[lane_rows(c), at] = value.T.astype(jnp.bfloat16)

    def make_sent(c):
        for i in range(1, ys):
            make((y + i) % ys, c, g_send.at[i - 1])

    def make_own(c):
        make(y, c, gathered.at[tensor, y])
        partner_copy(tensor, y, c).start()

    def send_y(c):
        for i in range(1, ys):
            y_copy(i, c).start()

    def send_x(part, c):
        for n in range(1, xs):
            x_copy(n, part, c).start()

    def send_attn():
        for k in range(strips):
            for i in range(1, ys):
                attn_copy(i, k).start()

    def relay_y(c):
        for i in range(1, ys):
            part = (y + i) % ys
            arrive(tensor, part, c)
            partner_copy(tensor, part, c).start()
            send_x(part, c)

    others = [((x + n) % xs) * 2 for n in range(1, xs)]

    def relay_x(part, c, when):
        for other in others:
            @pl.when(when(other + core))
            def _():
                arrive(other + core, part, c)
                partner_copy(other + core, part, c).start()

    messages = [(0, early, k, k + 1) for k in range(strips)]
    halves = [(0, strips // 2), (strips // 2, strips)] if strips > 1 else [(0, strips)]
    rest = chunks - early
    late = [(c, 1) + half for c in range(early, chunks) for half in halves]
    soon = [(early, rest, 0, two)] + [(early, rest, k, k + 1) for k in range(two, strips)] if rest else []
    late_ids = range(strips, strips + len(late))
    soon_ids = range(strips + len(late), strips + len(late) + len(soon))
    messages = messages + late + soon

    def window(m):
        c, count, k_first, k_end = messages[m]
        return pl.ds(k_first, k_end - k_first), pl.ds(c * LANES, LANES * count)

    def right_copy(slot, m):
        ks, at = window(m)
        return pltpu.make_async_remote_copy(
            src_ref=z_send.at[slot, ks, at, :], dst_ref=z_left.at[slot, ks, at, :],
            send_sem=z_send_sem.at[slot, m], recv_sem=zl_sem.at[slot, m],
            device_id={"dp": dp + ys}, device_id_type=mesh_id,
        )

    def left_copy(slot, m):
        ks, at = window(m)
        return pltpu.make_async_remote_copy(
            src_ref=z_send.at[slot, ks, at, :], dst_ref=z_right.at[slot, ks, at, :],
            send_sem=z_send_sem.at[slot, m], recv_sem=zr_sem.at[slot, m],
            device_id={"dp": dp - ys}, device_id_type=mesh_id,
        )

    def product(slot, k, c, count, width=1):
        at = pl.ds(c * LANES, LANES * count)
        left = jnp.concatenate([gathered[slot, part, at, :] for part in range(ys)], axis=1)
        right = jnp.concatenate([attn[k + n] for n in range(width)], axis=1)
        value = jnp.dot(left, right, preferred_element_type=jnp.float32)
        return [value[:, n * LANES : (n + 1) * LANES] for n in range(width)]

    def compute(slot, m):
        c, count, k_first, k_end = messages[m]
        at = pl.ds(c * LANES, LANES * count)
        rightmost, leftmost = (slot > z) & (z == 0), (slot < z) & (z == zs - 1)

        width = 2 - (k_end - k_first) % 2

        @pl.loop(k_first, k_end, step=width)
        def _(k):
            values = product(slot, k, c, count, width)

            @pl.when(rightmost | leftmost)
            def _():
                for n, value in enumerate(values):
                    z_send[slot, k + n, at, :] = value.astype(jnp.bfloat16)

            @pl.when(jnp.logical_not(rightmost | leftmost))
            def _():
                for n, value in enumerate(values):
                    own[slot, k + n, at, :] = value

        @pl.when(rightmost)
        def _():
            right_copy(slot, m).start()

        @pl.when(leftmost)
        def _():
            left_copy(slot, m).start()

    def pass_on(slot, m, hop):
        c, count, k_first, k_end = messages[m]
        at = pl.ds(c * LANES, LANES * count)

        @pl.when((slot > z) & (z == hop))
        def _():
            right_copy(slot, m).wait_recv()
            for k in range(k_first, k_end):
                value = own[slot, k, at, :] + z_left[slot, k, at, :].astype(jnp.float32)
                z_send[slot, k, at, :] = value.astype(jnp.bfloat16)
            right_copy(slot, m).start()

        @pl.when((slot < z) & (z == zs - 1 - hop))
        def _():
            left_copy(slot, m).wait_recv()
            for k in range(k_first, k_end):
                value = own[slot, k, at, :] + z_right[slot, k, at, :].astype(jnp.float32)
                z_send[slot, k, at, :] = value.astype(jnp.bfloat16)
            left_copy(slot, m).start()

    pairs = [(i, j) for i in range(depth) for j in range(min(i + 2, depth + 1))]
    quarters = 4

    def coef_partial(quarter):
        size = tokens // 16 // quarters

        def step(r, sums):
            at = pl.ds(pl.multiple_of(r * 16, 16), 16)
            sums = list(sums)
            for col in range(features // LANES):
                lanes = slice(col * LANES, (col + 1) * LANES)
                g = [grads[i, at, lanes].astype(jnp.float32) for i in range(depth)]
                o = [outs[j, at, lanes].astype(jnp.float32) for j in range(depth + 1)]
                for n, (i, j) in enumerate(pairs):
                    value = g[i] * o[j]
                    sums[n] += value[:8] + value[8:]
            return tuple(sums)

        zero = jnp.zeros((8, LANES), jnp.float32)
        first = tuple(zero if quarter == 0 else sums_ref[n] for n in range(len(pairs)))
        sums = lax.fori_loop(quarter * size, (quarter + 1) * size, step, first)
        for n in range(len(pairs)):
            sums_ref[n] = sums[n]

    def coef_tile():
        row = lax.broadcasted_iota(jnp.int32, (8, LANES), 0)
        col = lax.broadcasted_iota(jnp.int32, (8, LANES), 1)
        tile = jnp.zeros((8, LANES), jnp.float32)
        for n, (i, j) in enumerate(pairs):
            value = jnp.sum(sums_ref[n], axis=(0, 1), keepdims=True)
            tile = jnp.where((row == i) & (col == j), value, tile)
        return tile

    def coef_hop(stage, target):
        return pltpu.make_async_remote_copy(
            src_ref=coef_a.at[stage], dst_ref=coef_b.at[stage],
            send_sem=ca_send.at[stage], recv_sem=ca_recv.at[stage],
            device_id=target, device_id_type=mesh_id,
        )

    def coef_step(step):
        if step < zs:
            @pl.when(z == step)
            def _():
                coef_a[0] = coef_tile()
                if step > 0:
                    coef_hop(0, {"dp": dp + ys}).wait_recv()
                    coef_a[0] += coef_b[0]
                if step < zs - 1:
                    coef_hop(0, {"dp": dp + ys}).start()
                else:
                    coef_a[1] = coef_a[0]
                    coef_hop(1, {"dp": dp - ys}).start()
        else:
            plane = 2 * zs - 2 - step

            @pl.when(z == plane)
            def _():
                coef_hop(1, {"dp": dp - ys}).wait_recv()
                coef_a[1] = coef_b[1]
                if plane > 0:
                    coef_hop(1, {"dp": dp - ys}).start()

    def coef_partner(start):
        if start:
            coef_hop(2, {"tensor": partner}).start()
        else:
            coef_hop(2, {"tensor": partner}).wait_recv()

    def coef_x(n, at):
        return pltpu.make_async_remote_copy(
            src_ref=coef_c.at[at], dst_ref=coef_c.at[at],
            send_sem=cb_send.at[n], recv_sem=cb_recv.at[at],
            device_id={"tensor": (x + n) % xs * 2 + core}, device_id_type=mesh_id,
        )

    def coef_y(i, at):
        return pltpu.make_async_remote_copy(
            src_ref=coef_c.at[xs + at], dst_ref=coef_c.at[xs + at],
            send_sem=cb_send.at[xs + i], recv_sem=cb_recv.at[xs + at],
            device_id={"dp": z * ys + (y + i) % ys}, device_id_type=mesh_id,
        )

    last = tensor == z
    first = tensor == beside
    plain = jnp.logical_not(last | first)
    sooner = jnp.logical_not(last)
    parts = [y] + [(y + i) % ys for i in range(1, ys)]

    def away(slot):
        return slot != z

    def away_first(slot):
        return (slot != z) & first

    def away_plain(slot):
        return (slot != z) & jnp.logical_not(first)

    def home(slot):
        return slot == z

    def never(slot):
        return slot < 0

    def near(slot):
        return (slot != z) & (slot // 2 == x)

    def far(slot):
        return (slot != z) & (slot // 2 != x)

    def is_first(slot):
        return slot == beside

    def is_plain(slot):
        return (slot != z) & (slot != beside)

    def near_plain(slot):
        return near(slot) & (slot != beside)

    def far_plain(slot):
        return far(slot) & (slot != beside)

    def near_first(slot):
        return (slot == beside) & (slot // 2 == x)

    def far_first(slot):
        return (slot == beside) & (slot // 2 != x)

    def slot_at(i):
        outer = jnp.where(i % 2 == 0, zs - 1 - i // 2, i // 2)
        return jnp.where(z < zs // 2, outer, zs - 1 - outer)

    queue, clock = [], [0]

    def tick():
        for hop in range(1, zs - 1):
            index = clock[0] - LAG - (hop - 1) * SKEW
            if 0 <= index < len(queue):
                follow(*queue[index], hop)
        clock[0] += 1

    def follow(m, passed, hop):
        @pl.loop(0, zs)
        def _(i):
            slot = slot_at(i)

            @pl.when(passed(slot))
            def _():
                pass_on(slot, m, hop)

    def run(m, when, passed):
        @pl.loop(0, zs)
        def _(i):
            slot = slot_at(i)

            @pl.when(when(slot))
            def _():
                compute(slot, m)

        if passed is not never:
            queue.append((m, passed))
            tick()

    def gather_partner(slot, c_first, c_end, when):
        @pl.when(when(slot))
        def _():
            for c in range(c_first, c_end):
                for part in parts:
                    arrive(slot, part, c)

    steps = list(range(2 * zs - 1))
    share = -(-len(steps) // 7)

    def coef_steps():
        for step in steps[:share]:
            coef_step(step)
        del steps[:share]

    loads[0].wait()
    loads[1].wait()
    make_sent(0)
    meet()

    @pl.when(sooner)
    def _():
        send_y(0)

    make_own(0)

    @pl.when(sooner)
    def _():
        send_x(y, 0)

    for c in range(1, early):
        make_sent(c)

        @pl.when(sooner)
        def _():
            send_y(c)

    @pl.when(first)
    def _():
        for c in range(early, chunks):
            make_sent(c)
            send_y(c)

    for load in attn_loads:
        load.wait()
    send_attn()
    for c in range(1, early):
        make_own(c)
    for load in loads[2:]:
        load.wait()

    coef_partial(0)
    for c in range(early):
        @pl.when(sooner)
        def _():
            relay_y(c)
            if c + 1 < early:
                send_x(y, c + 1)

        if c == 0:
            relay_x(y, 0, away)
        coef_partial(1 + c if early > 1 else 1)
    for quarter in range(1 + max(early, 1), quarters):
        coef_partial(quarter)
    coef_steps()
    for part in parts[1:]:
        relay_x(part, 0, away)

    @pl.when(first)
    def _():
        for c in range(early, chunks):
            make_own(c)
            send_x(y, c)
            relay_y(c)

    for c in range(1, early):
        relay_x(y, c, away_first)

    attn_arrive(0)
    gather_partner(partner, 0, early, away)
    run(0, near, near)
    coef_steps()
    for c in range(1, early):
        relay_x(y, c, away_plain)
        for part in parts[1:]:
            relay_x(part, c, away_first)
    coef_steps()
    if two > 1:
        attn_arrive(1)
        run(1, near, near)
    coef_steps()
    for c in range(1, early):
        for part in parts[1:]:
            relay_x(part, c, away_plain)
    soon_left = list(soon_ids)
    if rest:
        gather_partner(partner, early, chunks, is_first)
        run(soon_left[0], near_first, never)
    for other in others:
        gather_partner(other + 1 - core, 0, early, away)
    for k in range(two):
        run(k, far, far)
    if rest:
        for c in range(early, chunks):
            for part in parts:
                relay_x(part, c, is_first)
        for other in others:
            gather_partner(other + 1 - core, early, chunks, is_first)
        run(soon_left.pop(0), far_first, never)

        @pl.when(plain | last)
        def _():
            for c in range(early, chunks):
                make_sent(c)

        @pl.when(plain)
        def _():
            for c in range(early, chunks):
                send_y(c)

        @pl.when(plain | last)
        def _():
            for c in range(early, chunks):
                make_own(c)

        @pl.when(plain)
        def _():
            for c in range(early, chunks):
                send_x(y, c)

    @pl.when(last)
    def _():
        for c in range(chunks):
            send_y(c)

    for k in range(two, strips):
        attn_arrive(k)
        run(k, away, away)
        if soon_left:
            run(soon_left.pop(0), is_first, never)
        if k % 2:
            coef_steps()
        if k == strips // 2:
            @pl.when(last)
            def _():
                for c in range(chunks):
                    send_x(y, c)
    while steps:
        coef_steps()
    coef_a[2] = coef_a[1]
    coef_partner(True)

    for c in range(early, chunks):
        relay_x(y, c, is_plain)
    for c in range(chunks):
        relay_x(y, c, home)
    behind = list(range(chunks))
    for c in range(early, chunks):
        @pl.when(plain)
        def _():
            relay_y(c)

        now, behind = behind[: -(-chunks // max(rest, 1))], behind[-(-chunks // max(rest, 1)):]

        @pl.when(last)
        def _():
            for d in now:
                relay_y(d)

        gather_partner(partner, c, c + 1, is_plain)
        for h in range(len(halves)):
            run(late_ids[(c - early) * len(halves) + h], near_plain, near)

    @pl.when(last)
    def _():
        for d in behind:
            relay_y(d)

    for c in range(early, chunks):
        for part in parts[1:]:
            relay_x(part, c, is_plain)
        if c == early:
            coef_partner(False)
            coef_c[x] = coef_a[2] + coef_b[2]
            for n in range(1, xs):
                coef_x(n, x).start()
        for other in others:
            gather_partner(other + 1 - core, c, c + 1, is_plain)
        for h in range(len(halves)):
            run(late_ids[(c - early) * len(halves) + h], far_plain, far)
    if not rest:
        coef_partner(False)
        coef_c[x] = coef_a[2] + coef_b[2]
        for n in range(1, xs):
            coef_x(n, x).start()
    for n in range(1, xs):
        coef_x(n, (x + n) % xs).wait_recv()
    total = coef_c[0]
    for n in range(1, xs):
        total += coef_c[n]
    coef_c[xs + y] = total
    for i in range(1, ys):
        coef_y(i, y).start()

    for c in range(chunks):
        for part in parts[1:]:
            relay_x(part, c, home)
    for _ in range(LAG + (zs - 3) * SKEW):
        tick()

    @pl.when(z % 2 != core)
    def _():
        for c in range(chunks):
            for part in parts:
                arrive(z, part, c)

    width = 2 - strips % 2

    @pl.loop(0, strips, step=width)
    def _(k):
        for n, value in enumerate(product(z, k, 0, chunks, width)):
            own[z, k + n] = value

    for i in range(1, ys):
        coef_y(i, (y + i) % ys).wait_recv()
    total = coef_c[xs]
    for i in range(1, ys):
        total += coef_c[xs + i]
    coef_out[...] = total[: coef_out.shape[0], : coef_out.shape[1]]

    def from_left(ids):
        for m in ids:
            right_copy(z, m).wait_recv()

    def from_right(ids):
        for m in ids:
            left_copy(z, m).wait_recv()

    @pl.when(z > 0)
    def _():
        from_left(range(strips))

    @pl.when(z < zs - 1)
    def _():
        from_right(range(strips))

    if rest:
        @pl.when(z == 1)
        def _():
            from_left(soon_ids)

        @pl.when(z > 1)
        def _():
            from_left(late_ids)

        @pl.when(z == zs - 2)
        def _():
            from_right(soon_ids)

        @pl.when(z < zs - 2)
        def _():
            from_right(late_ids)

    for k in range(strips):
        lanes = slice(k * LANES, (k + 1) * LANES)
        proj_out[:, lanes] = own[z, k]

        @pl.when(z > 0)
        def _():
            proj_out[:, lanes] += z_left[z, k].astype(jnp.float32)

        @pl.when(z < zs - 1)
        def _():
            proj_out[:, lanes] += z_right[z, k].astype(jnp.float32)

    @pl.loop(0, zs)
    def _(slot):
        @pl.when(slot != z)
        def _():
            for m in range(strips):
                right_copy(slot, m).wait_send()

        @pl.when(slot == beside)
        def _():
            for m in soon_ids:
                right_copy(slot, m).wait_send()

        @pl.when(is_plain(slot))
        def _():
            for m in late_ids:
                right_copy(slot, m).wait_send()

    for c in range(chunks):
        for i in range(1, ys):
            y_copy(i, c).wait_send()
        for part in range(ys):
            for n in range(xs):
                partner_copy(n * 2 + core, part, c).wait_send()
            for n in range(1, xs):
                x_copy(n, part, c).wait_send()
    for k in range(strips):
        for i in range(1, ys):
            attn_copy(i, k).wait_send()

    @pl.when(z < zs - 1)
    def _():
        coef_hop(0, {"dp": dp + ys}).wait_send()

    @pl.when(z > 0)
    def _():
        coef_hop(1, {"dp": dp - ys}).wait_send()

    coef_hop(2, {"tensor": partner}).wait_send()
    for n in range(1, xs):
        coef_x(n, x).wait_send()
    for i in range(1, ys):
        coef_y(i, y).wait_send()


def local(dp_size, tensor_size, layer_outs, avg_grads, attn_mixed, dwa_coefs):
    depth, tokens, features = avg_grads.shape
    rows = features * tensor_size // dp_size
    cols = attn_mixed.shape[1]
    ys, zs, xs = dp_size // tensor_size, tensor_size, tensor_size // 2
    strips, chunks = cols // LANES, rows // LANES
    bf16, f32 = jnp.bfloat16, jnp.float32
    dma = pltpu.SemaphoreType.DMA
    any_space = pl.BlockSpec(memory_space=pl.ANY)
    vmem = pl.BlockSpec(memory_space=pltpu.VMEM)
    return pl.pallas_call(
        functools.partial(kernel, dp_size, tensor_size),
        out_shape=(
            jax.ShapeDtypeStruct(dwa_coefs.shape, f32),
            jax.ShapeDtypeStruct((rows, cols), f32),
        ),
        in_specs=[any_space, any_space, any_space, pl.BlockSpec(memory_space=pltpu.SMEM)],
        out_specs=(vmem, vmem),
        scratch_shapes=[
            pltpu.VMEM(layer_outs.shape, bf16),
            pltpu.VMEM(avg_grads.shape, bf16),
            pltpu.VMEM((strips, ys * tokens, LANES), bf16),
            pltpu.VMEM((zs, ys, rows, tokens), bf16),
            pltpu.VMEM((ys - 1, rows, tokens), bf16),
            pltpu.VMEM((zs, strips, rows, LANES), f32),
            pltpu.VMEM((zs, strips, rows, LANES), bf16),
            pltpu.VMEM((zs, strips, rows, LANES), bf16),
            pltpu.VMEM((zs, strips, rows, LANES), bf16),
            pltpu.VMEM((depth * (depth + 1), 8, LANES), f32),
            pltpu.VMEM((3, 8, LANES), f32),
            pltpu.VMEM((3, 8, LANES), f32),
            pltpu.VMEM((xs + ys, 8, LANES), f32),
            dma((2 * depth + 1,)),
            dma((strips,)),
            dma((ys - 1, chunks)),
            dma((xs, ys, chunks)),
            dma((max(xs - 1, 1), ys, chunks)),
            dma((tensor_size, ys, chunks)),
            dma((ys - 1, strips)),
            dma((ys, strips)),
            dma((zs, 2 * strips + 2 * chunks)),
            dma((zs, 2 * strips + 2 * chunks)),
            dma((zs, 2 * strips + 2 * chunks)),
            dma((3,)),
            dma((3,)),
            dma((xs + ys,)),
            dma((xs + ys,)),
        ],
        compiler_params=pltpu.CompilerParams(
            collective_id=0, has_side_effects=True, vmem_limit_bytes=67000000
        ),
    )(layer_outs, avg_grads, attn_mixed, dwa_coefs)


def solution(mesh):
    sizes = (mesh.shape["dp"], mesh.shape["tensor"])
    in_specs = (P(None, "dp", "tensor"), P(None, "dp", "tensor"), P("dp", "tensor"), P())
    out_specs = (P(), P("dp", "tensor"))
    return jax.shard_map(
        functools.partial(local, *sizes), mesh=mesh, in_specs=in_specs, out_specs=out_specs, check_vma=False
    )
```

```python
import functools

import jax
import jax.numpy as jnp
from jax import lax
from jax.experimental import pallas as pl
from jax.experimental.pallas import tpu as pltpu
from jax.sharding import PartitionSpec as P

LANES = 128
LAG = 1
SKEW = 2


def kernel(
    dp_size, tensor_size, outs_hbm, grads_hbm, attn_hbm, coefs, coef_out, proj_out,
    outs, grads, attn, gathered, g_send, own, z_send, z_left, z_right, sums_ref, coef_a, coef_b, coef_c, result,
    load_sem, attn_sem, gy_sem, p_sem, x_sem, g_recv, a_sem, a_recv,
    z_send_sem, z_sem, ca_send, ca_recv, cb_send, cb_recv,
):
    depth, tokens, features = grads.shape
    rows, cols = result.shape
    strips = cols // LANES
    chunks = rows // LANES
    early = max(chunks // 2, 1)
    ys = dp_size // tensor_size
    zs = tensor_size
    xs = tensor_size // 2
    dp, tensor = lax.axis_index("dp"), lax.axis_index("tensor")
    z, y = dp // ys, dp % ys
    x, core = tensor // 2, tensor % 2
    partner = x * 2 + 1 - core
    beside = jnp.where(z == 0, 1, jnp.where(z == zs - 1, zs - 2, -1))
    two = min(2, strips)
    mesh_id = pl.DeviceIdType.MESH

    loads = []
    for i in (depth - 2, depth - 1):
        loads.append(pltpu.make_async_copy(grads_hbm.at[i], grads.at[i], load_sem.at[i]))
    for i in range(depth - 2):
        loads.append(pltpu.make_async_copy(grads_hbm.at[i], grads.at[i], load_sem.at[i]))
    for j in range(depth + 1):
        loads.append(pltpu.make_async_copy(outs_hbm.at[j], outs.at[j], load_sem.at[depth + j]))
    mine = pl.ds(pl.multiple_of(y * tokens, tokens), tokens)
    attn_loads = [
        pltpu.make_async_copy(
            attn_hbm.at[:, pl.ds(k * LANES, LANES)], attn.at[k, mine, :], attn_sem
        )
        for k in range(strips)
    ]
    loads[0].start()
    loads[1].start()
    for load in attn_loads:
        load.start()
    for load in loads[2:]:
        load.start()

    barrier = pltpu.get_barrier_semaphore()

    def greet(**device):
        pl.semaphore_signal(barrier, inc=1, device_id=device, device_id_type=mesh_id)

    greet(tensor=partner)
    for i in range(1, ys):
        greet(dp=z * ys + (y + i) % ys)
    for n in range(1, xs):
        greet(tensor=(x + n) % xs * 2 + core)

    @pl.when(z > 0)
    def _():
        greet(dp=dp - ys)

    @pl.when(z < zs - 1)
    def _():
        greet(dp=dp + ys)

    def meet():
        ends = jnp.where(z == 0, 1, 0) + jnp.where(z == zs - 1, 1, 0)
        pl.semaphore_wait(barrier, 1 + (ys - 1) + (xs - 1) + 2 - ends)

    def lane_rows(c, count=1):
        return pl.ds(c * LANES, LANES * count)

    def piece(slot, part, c):
        return gathered.at[slot, part, lane_rows(c), :]

    def y_copy(i, c):
        return pltpu.make_async_remote_copy(
            src_ref=g_send.at[i - 1, lane_rows(c), :], dst_ref=piece(tensor, y, c),
            send_sem=gy_sem.at[i - 1], recv_sem=g_recv.at[tensor, y, c],
            device_id={"dp": z * ys + (y + i) % ys}, device_id_type=mesh_id,
        )

    def partner_copy(slot, part, c):
        return pltpu.make_async_remote_copy(
            src_ref=piece(slot, part, c), dst_ref=piece(slot, part, c),
            send_sem=p_sem.at[slot // 2], recv_sem=g_recv.at[slot, part, c],
            device_id={"tensor": partner}, device_id_type=mesh_id,
        )

    def x_copy(n, part, c):
        return pltpu.make_async_remote_copy(
            src_ref=piece(tensor, part, c), dst_ref=piece(tensor, part, c),
            send_sem=x_sem.at[n - 1], recv_sem=g_recv.at[tensor, part, c],
            device_id={"tensor": (x + n) % xs * 2 + core}, device_id_type=mesh_id,
        )

    def arrive(slot, part, c):
        partner_copy(slot, part, c).wait_recv()

    def attn_copy(i, k):
        return pltpu.make_async_remote_copy(
            src_ref=attn.at[k, mine, :], dst_ref=attn.at[k, mine, :],
            send_sem=a_sem.at[i - 1], recv_sem=a_recv.at[ys - i - 1, k],
            device_id={"dp": z * ys + (y + i) % ys}, device_id_type=mesh_id,
        )

    def attn_arrive(k):
        for i in range(1, ys):
            part = (y + i) % ys
            there = pl.ds(pl.multiple_of(part * tokens, tokens), tokens)
            pltpu.make_async_remote_copy(
                src_ref=attn.at[k, there, :], dst_ref=attn.at[k, there, :],
                send_sem=a_sem.at[i - 1], recv_sem=a_recv.at[i - 1, k],
                device_id={"dp": z * ys + part}, device_id_type=mesh_id,
            ).wait_recv()

    def make(part, c, into):
        first, second = coefs[depth - 2, depth - 1], coefs[depth - 1, depth - 1]

        @pl.loop(0, tokens // LANES)
        def _(step):
            at = pl.ds(pl.multiple_of(step * LANES, LANES), LANES)
            wide = pl.ds(pl.multiple_of(part * rows + c * LANES, LANES), LANES)
            value = first * grads[depth - 2, at, wide].astype(jnp.float32)
            value += second * grads[depth - 1, at, wide].astype(jnp.float32)
            into[lane_rows(c), at] = value.T.astype(jnp.bfloat16)

    def make_sent(c):
        for i in range(1, ys):
            make((y + i) % ys, c, g_send.at[i - 1])

    def make_own(c):
        make(y, c, gathered.at[tensor, y])
        partner_copy(tensor, y, c).start()

    def send_y(c):
        for i in range(1, ys):
            y_copy(i, c).start()

    def send_x(part, c):
        for n in range(1, xs):
            x_copy(n, part, c).start()

    def send_attn():
        for k in range(strips):
            for i in range(1, ys):
                attn_copy(i, k).start()

    def relay_y(c):
        for i in range(1, ys):
            part = (y + i) % ys
            arrive(tensor, part, c)
            partner_copy(tensor, part, c).start()
            send_x(part, c)

    others = [((x + n) % xs) * 2 for n in range(1, xs)]

    def relay_x(part, c, when):
        for other in others:
            @pl.when(when(other + core))
            def _():
                arrive(other + core, part, c)
                partner_copy(other + core, part, c).start()

    messages = [(0, early, k, k + 1) for k in range(strips)]
    halves = [(0, strips // 2), (strips // 2, strips)] if strips > 1 else [(0, strips)]
    rest = chunks - early
    late = [(c, 1) + half for c in range(early, chunks) for half in halves]
    soon = [(early, rest, 0, two)] + [(early, rest, k, k + 1) for k in range(two, strips)] if rest else []
    late_ids = range(strips, strips + len(late))
    soon_ids = range(strips + len(late), strips + len(late) + len(soon))
    messages = messages + late + soon

    def window(m):
        c, count, k_first, k_end = messages[m]
        return pl.ds(k_first, k_end - k_first), pl.ds(c * LANES, LANES * count)

    passing = strips + len(late)

    def arrival(slot, m):
        return slot * passing + m

    def right_copy(slot, m, sem):
        ks, at = window(m)
        return pltpu.make_async_remote_copy(
            src_ref=z_send.at[slot, ks, at, :], dst_ref=z_left.at[slot, ks, at, :],
            send_sem=z_send_sem.at[slot], recv_sem=z_sem.at[sem],
            device_id={"dp": dp + ys}, device_id_type=mesh_id,
        )

    def left_copy(slot, m, sem):
        ks, at = window(m)
        return pltpu.make_async_remote_copy(
            src_ref=z_send.at[slot, ks, at, :], dst_ref=z_right.at[slot, ks, at, :],
            send_sem=z_send_sem.at[slot], recv_sem=z_sem.at[sem],
            device_id={"dp": dp - ys}, device_id_type=mesh_id,
        )

    def send_right(slot, m):
        sem = zs * passing if m in soon_ids else jnp.where(slot == z + 1, zs * passing, arrival(slot, m))
        right_copy(slot, m, sem).start()

    def send_left(slot, m):
        sem = zs * passing + 1 if m in soon_ids else jnp.where(slot == z - 1, zs * passing + 1, arrival(slot, m))
        left_copy(slot, m, sem).start()

    def product(slot, k, c, count, width=1):
        at = pl.ds(c * LANES, LANES * count)
        left = jnp.concatenate([gathered[slot, part, at, :] for part in range(ys)], axis=1)
        right = jnp.concatenate([attn[k + n] for n in range(width)], axis=1)
        value = jnp.dot(left, right, preferred_element_type=jnp.float32)
        return [value[:, n * LANES : (n + 1) * LANES] for n in range(width)]

    def compute(slot, m):
        c, count, k_first, k_end = messages[m]
        at = pl.ds(c * LANES, LANES * count)
        rightmost, leftmost = (slot > z) & (z == 0), (slot < z) & (z == zs - 1)

        width = 2 - (k_end - k_first) % 2

        @pl.loop(k_first, k_end, step=width)
        def _(k):
            values = product(slot, k, c, count, width)

            @pl.when(rightmost | leftmost)
            def _():
                for n, value in enumerate(values):
                    z_send[slot, k + n, at, :] = value.astype(jnp.bfloat16)

            @pl.when(jnp.logical_not(rightmost | leftmost))
            def _():
                for n, value in enumerate(values):
                    own[slot, k + n, at, :] = value

        @pl.when(rightmost)
        def _():
            send_right(slot, m)

        @pl.when(leftmost)
        def _():
            send_left(slot, m)

    def pass_on(slot, m, hop):
        c, count, k_first, k_end = messages[m]
        at = pl.ds(c * LANES, LANES * count)

        @pl.when((slot > z) & (z == hop))
        def _():
            right_copy(slot, m, arrival(slot, m)).wait_recv()
            for k in range(k_first, k_end):
                value = own[slot, k, at, :] + z_left[slot, k, at, :].astype(jnp.float32)
                z_send[slot, k, at, :] = value.astype(jnp.bfloat16)
            send_right(slot, m)

        @pl.when((slot < z) & (z == zs - 1 - hop))
        def _():
            left_copy(slot, m, arrival(slot, m)).wait_recv()
            for k in range(k_first, k_end):
                value = own[slot, k, at, :] + z_right[slot, k, at, :].astype(jnp.float32)
                z_send[slot, k, at, :] = value.astype(jnp.bfloat16)
            send_left(slot, m)

    pairs = [(i, j) for i in range(depth) for j in range(min(i + 2, depth + 1))]
    quarters = 4

    def coef_partial(quarter):
        size = tokens // 16 // quarters

        def step(r, sums):
            at = pl.ds(pl.multiple_of(r * 16, 16), 16)
            sums = list(sums)
            for col in range(features // LANES):
                lanes = slice(col * LANES, (col + 1) * LANES)
                g = [grads[i, at, lanes].astype(jnp.float32) for i in range(depth)]
                o = [outs[j, at, lanes].astype(jnp.float32) for j in range(depth + 1)]
                for n, (i, j) in enumerate(pairs):
                    value = g[i] * o[j]
                    sums[n] += value[:8] + value[8:]
            return tuple(sums)

        zero = jnp.zeros((8, LANES), jnp.float32)
        first = tuple(zero if quarter == 0 else sums_ref[n] for n in range(len(pairs)))
        sums = lax.fori_loop(quarter * size, (quarter + 1) * size, step, first)
        for n in range(len(pairs)):
            sums_ref[n] = sums[n]

    def coef_tile():
        row = lax.broadcasted_iota(jnp.int32, (8, LANES), 0)
        col = lax.broadcasted_iota(jnp.int32, (8, LANES), 1)
        tile = jnp.zeros((8, LANES), jnp.float32)
        for n, (i, j) in enumerate(pairs):
            value = jnp.sum(sums_ref[n], axis=(0, 1), keepdims=True)
            tile = jnp.where((row == i) & (col == j), value, tile)
        return tile

    def coef_hop(stage, target):
        return pltpu.make_async_remote_copy(
            src_ref=coef_a.at[stage], dst_ref=coef_b.at[stage],
            send_sem=ca_send.at[stage], recv_sem=ca_recv.at[stage],
            device_id=target, device_id_type=mesh_id,
        )

    def coef_step(step):
        if step < zs:
            @pl.when(z == step)
            def _():
                coef_a[0] = coef_tile()
                if step > 0:
                    coef_hop(0, {"dp": dp + ys}).wait_recv()
                    coef_a[0] += coef_b[0]
                if step < zs - 1:
                    coef_hop(0, {"dp": dp + ys}).start()
                else:
                    coef_a[1] = coef_a[0]
                    coef_hop(1, {"dp": dp - ys}).start()
        else:
            plane = 2 * zs - 2 - step

            @pl.when(z == plane)
            def _():
                coef_hop(1, {"dp": dp - ys}).wait_recv()
                coef_a[1] = coef_b[1]
                if plane > 0:
                    coef_hop(1, {"dp": dp - ys}).start()

    def coef_partner(start):
        if start:
            coef_hop(2, {"tensor": partner}).start()
        else:
            coef_hop(2, {"tensor": partner}).wait_recv()

    def coef_x(n, at):
        return pltpu.make_async_remote_copy(
            src_ref=coef_c.at[at], dst_ref=coef_c.at[at],
            send_sem=cb_send.at[n], recv_sem=cb_recv.at[at],
            device_id={"tensor": (x + n) % xs * 2 + core}, device_id_type=mesh_id,
        )

    def coef_y(i, at):
        return pltpu.make_async_remote_copy(
            src_ref=coef_c.at[xs + at], dst_ref=coef_c.at[xs + at],
            send_sem=cb_send.at[xs + i], recv_sem=cb_recv.at[xs + at],
            device_id={"dp": z * ys + (y + i) % ys}, device_id_type=mesh_id,
        )

    last = tensor == z
    first = tensor == beside
    plain = jnp.logical_not(last | first)
    sooner = jnp.logical_not(last)
    parts = [y] + [(y + i) % ys for i in range(1, ys)]

    def away(slot):
        return slot != z

    def away_first(slot):
        return (slot != z) & first

    def away_plain(slot):
        return (slot != z) & jnp.logical_not(first)

    def home(slot):
        return slot == z

    def never(slot):
        return slot < 0

    def near(slot):
        return (slot != z) & (slot // 2 == x)

    def far(slot):
        return (slot != z) & (slot // 2 != x)

    def is_first(slot):
        return slot == beside

    def is_plain(slot):
        return (slot != z) & (slot != beside)

    def near_plain(slot):
        return near(slot) & (slot != beside)

    def far_plain(slot):
        return far(slot) & (slot != beside)

    def near_first(slot):
        return (slot == beside) & (slot // 2 == x)

    def far_first(slot):
        return (slot == beside) & (slot // 2 != x)

    def slot_at(i):
        outer = jnp.where(i % 2 == 0, zs - 1 - i // 2, i // 2)
        return jnp.where(z < zs // 2, outer, zs - 1 - outer)

    def late_of(c):
        return late_ids[(c - early) * len(halves) : (c - early + 1) * len(halves)]

    queue, done = [], {hop: 0 for hop in range(1, zs - 1)}

    def advance(hop, limit):
        while hop in done and done[hop] < min(limit, len(queue)):
            follow(*queue[done[hop]], hop)
            done[hop] += 1

    def tick():
        for hop in done:
            advance(hop, len(queue) - LAG - (hop - 1) * SKEW)

    def flush():
        while any(place < len(queue) for place in done.values()):
            for hop in done:
                ahead = done.get(hop - 1, len(queue))
                limit = ahead if ahead == len(queue) else ahead - 1
                advance(hop, min(done[hop] + hop, limit))

    def follow(ms, passed, hop):
        @pl.loop(0, zs)
        def _(i):
            slot = slot_at(i)

            @pl.when(passed(slot))
            def _():
                for m in ms:
                    pass_on(slot, m, hop)

    def run(ms, when, passed):
        @pl.loop(0, zs)
        def _(i):
            slot = slot_at(i)

            @pl.when(when(slot))
            def _():
                for m in ms:
                    compute(slot, m)

        if passed is not never:
            queue.append((ms, passed))

    def gather_partner(slot, c_first, c_end, when):
        @pl.when(when(slot))
        def _():
            for c in range(c_first, c_end):
                for part in parts:
                    arrive(slot, part, c)

    steps = list(range(2 * zs - 1))
    share = -(-len(steps) // 7)

    def coef_steps():
        for step in steps[:share]:
            coef_step(step)
        del steps[:share]

    loads[0].wait()
    loads[1].wait()
    make_sent(0)
    meet()

    @pl.when(sooner)
    def _():
        send_y(0)

    make_own(0)

    @pl.when(sooner)
    def _():
        send_x(y, 0)

    for c in range(1, early):
        make_sent(c)

        @pl.when(sooner)
        def _():
            send_y(c)

    @pl.when(first)
    def _():
        for c in range(early, chunks):
            make_sent(c)
            send_y(c)

    pltpu.make_async_copy(attn.at[:, mine, :], attn.at[:, mine, :], attn_sem).wait()
    send_attn()
    for c in range(1, early):
        make_own(c)
    for load in loads[2:]:
        load.wait()

    coef_partial(0)
    for c in range(early):
        @pl.when(sooner)
        def _():
            relay_y(c)
            if c + 1 < early:
                send_x(y, c + 1)

        if c == 0:
            relay_x(y, 0, away)
        coef_partial(1 + c if early > 1 else 1)
    for quarter in range(1 + max(early, 1), quarters):
        coef_partial(quarter)
    coef_steps()
    for part in parts[1:]:
        relay_x(part, 0, away)

    @pl.when(first)
    def _():
        for c in range(early, chunks):
            make_own(c)
            send_x(y, c)
            relay_y(c)

    for c in range(1, early):
        relay_x(y, c, away_first)

    attn_arrive(0)
    gather_partner(partner, 0, early, away)
    run([0], near, near)
    tick()
    coef_steps()
    for c in range(1, early):
        relay_x(y, c, away_plain)
        for part in parts[1:]:
            relay_x(part, c, away_first)
    coef_steps()
    if two > 1:
        attn_arrive(1)
        run([1], near, near)
        tick()
    coef_steps()
    for c in range(1, early):
        for part in parts[1:]:
            relay_x(part, c, away_plain)
    soon_left = list(soon_ids)
    if rest:
        gather_partner(partner, early, chunks, is_first)
        run([soon_left[0]], near_first, never)
    for other in others:
        gather_partner(other + 1 - core, 0, early, away)
    for k in range(two):
        run([k], far, far)
        tick()
    if rest:
        for c in range(early, chunks):
            for part in parts:
                relay_x(part, c, is_first)
        for other in others:
            gather_partner(other + 1 - core, early, chunks, is_first)
        run([soon_left.pop(0)], far_first, never)

        @pl.when(plain | last)
        def _():
            for c in range(early, chunks):
                make_sent(c)

        @pl.when(plain)
        def _():
            for c in range(early, chunks):
                send_y(c)

        @pl.when(plain | last)
        def _():
            for c in range(early, chunks):
                make_own(c)

        @pl.when(plain)
        def _():
            for c in range(early, chunks):
                send_x(y, c)

    @pl.when(last)
    def _():
        for c in range(chunks):
            send_y(c)

    for k in range(two, strips):
        attn_arrive(k)
        run([k], away, away)
        tick()
        if soon_left:
            run([soon_left.pop(0)], is_first, never)
        if k % 2:
            coef_steps()
        if k == two:
            @pl.when(last)
            def _():
                for c in range(chunks):
                    send_x(y, c)
    while steps:
        coef_steps()
    coef_a[2] = coef_a[1]
    coef_partner(True)

    for c in range(early, chunks):
        relay_x(y, c, is_plain)
    for c in range(chunks):
        relay_x(y, c, home)
    behind = list(range(chunks))
    started = len(queue)
    for c in range(early, chunks):
        @pl.when(plain)
        def _():
            relay_y(c)

        now, behind = behind[: -(-chunks // max(rest, 1))], behind[-(-chunks // max(rest, 1)):]

        @pl.when(last)
        def _():
            for d in now:
                relay_y(d)

        gather_partner(partner, c, c + 1, is_plain)
        run(late_of(c), near_plain, near)
        advance(1, len(queue) - LAG)

    @pl.when(last)
    def _():
        for d in behind:
            relay_y(d)

    advance(2, started)

    for c in range(early, chunks):
        for part in parts[1:]:
            relay_x(part, c, is_plain)
        if c == early:
            coef_partner(False)
            coef_c[x] = coef_a[2] + coef_b[2]
            for n in range(1, xs):
                coef_x(n, x).start()
        for other in others:
            gather_partner(other + 1 - core, c, c + 1, is_plain)
        run(late_of(c), far_plain, far)
        advance(1, len(queue) - LAG)
        advance(2, started + c - early)
    if not rest:
        coef_partner(False)
        coef_c[x] = coef_a[2] + coef_b[2]
        for n in range(1, xs):
            coef_x(n, x).start()
    for n in range(1, xs):
        coef_x(n, (x + n) % xs).wait_recv()
    total = coef_c[0]
    for n in range(1, xs):
        total += coef_c[n]
    coef_c[xs + y] = total
    for i in range(1, ys):
        coef_y(i, y).start()

    for c in range(chunks):
        for part in parts[1:]:
            relay_x(part, c, home)
    flush()

    @pl.when(z % 2 != core)
    def _():
        for c in range(chunks):
            for part in parts:
                arrive(z, part, c)

    width = 2 - strips % 2

    @pl.loop(0, strips, step=width)
    def _(k):
        for n, value in enumerate(product(z, k, 0, chunks, width)):
            own[z, k + n] = value

    for i in range(1, ys):
        coef_y(i, (y + i) % ys).wait_recv()
    total = coef_c[xs]
    for i in range(1, ys):
        total += coef_c[xs + i]
    coef_b[2] = total
    coef_store = pltpu.make_async_copy(coef_b.at[2], coef_out, load_sem.at[0])
    coef_store.start()

    @pl.when(z > 0)
    def _():
        pltpu.make_async_remote_copy(
            src_ref=z_left.at[z], dst_ref=z_left.at[z],
            send_sem=z_send_sem.at[z], recv_sem=z_sem.at[zs * passing],
            device_id={"dp": dp - ys}, device_id_type=mesh_id,
        ).wait_recv()

    @pl.when(z < zs - 1)
    def _():
        pltpu.make_async_remote_copy(
            src_ref=z_right.at[z], dst_ref=z_right.at[z],
            send_sem=z_send_sem.at[z], recv_sem=z_sem.at[zs * passing + 1],
            device_id={"dp": dp + ys}, device_id_type=mesh_id,
        ).wait_recv()

    for c in range(chunks):
        at = lane_rows(c)
        for k in range(strips):
            lanes = slice(k * LANES, (k + 1) * LANES)
            result[at, lanes] = own[z, k, at, :]

            @pl.when(z > 0)
            def _():
                result[at, lanes] += z_left[z, k, at, :].astype(jnp.float32)

            @pl.when(z < zs - 1)
            def _():
                result[at, lanes] += z_right[z, k, at, :].astype(jnp.float32)

        pltpu.make_async_copy(result.at[at, :], proj_out.at[at, :], attn_sem).start()

    @pl.loop(0, zs)
    def _(slot):
        @pl.when(slot != z)
        def _():
            pltpu.make_async_remote_copy(
                src_ref=z_send.at[slot], dst_ref=z_left.at[slot],
                send_sem=z_send_sem.at[slot], recv_sem=z_sem.at[0],
                device_id={"dp": z * ys + (y + 1) % ys}, device_id_type=mesh_id,
            ).wait_send()

    def sent(ref, sem):
        pltpu.make_async_remote_copy(
            src_ref=ref, dst_ref=ref, send_sem=sem, recv_sem=z_sem.at[0],
            device_id={"tensor": partner}, device_id_type=mesh_id,
        ).wait_send()

    for i in range(1, ys):
        sent(g_send.at[i - 1], gy_sem.at[i - 1])
        sent(attn.at[:, mine, :], a_sem.at[i - 1])
    for n in range(xs):
        sent(gathered.at[n * 2 + core], p_sem.at[n])
    for n in range(1, xs):
        sent(gathered.at[tensor], x_sem.at[n - 1])

    @pl.when(z < zs - 1)
    def _():
        coef_hop(0, {"dp": dp + ys}).wait_send()

    @pl.when(z > 0)
    def _():
        coef_hop(1, {"dp": dp - ys}).wait_send()

    coef_hop(2, {"tensor": partner}).wait_send()
    for n in range(1, xs):
        coef_x(n, x).wait_send()
    for i in range(1, ys):
        coef_y(i, y).wait_send()
    coef_store.wait()
    pltpu.make_async_copy(result, proj_out, attn_sem).wait()


def settle(coef, proj, coef_out, proj_out):
    coef_out[...] = coef[: coef_out.shape[0], : coef_out.shape[1]]
    proj_out[...] = proj[...]


def local(dp_size, tensor_size, layer_outs, avg_grads, attn_mixed, dwa_coefs):
    depth, tokens, features = avg_grads.shape
    rows = features * tensor_size // dp_size
    cols = attn_mixed.shape[1]
    ys, zs, xs = dp_size // tensor_size, tensor_size, tensor_size // 2
    strips, chunks = cols // LANES, rows // LANES
    bf16, f32 = jnp.bfloat16, jnp.float32
    dma = pltpu.SemaphoreType.DMA
    any_space = pl.BlockSpec(memory_space=pl.ANY)
    coef, proj = pl.pallas_call(
        functools.partial(kernel, dp_size, tensor_size),
        out_shape=(
            jax.ShapeDtypeStruct((8, LANES), f32),
            jax.ShapeDtypeStruct((rows, cols), f32),
        ),
        in_specs=[any_space, any_space, any_space, pl.BlockSpec(memory_space=pltpu.SMEM)],
        out_specs=(any_space, any_space),
        scratch_shapes=[
            pltpu.VMEM(layer_outs.shape, bf16),
            pltpu.VMEM(avg_grads.shape, bf16),
            pltpu.VMEM((strips, ys * tokens, LANES), bf16),
            pltpu.VMEM((zs, ys, rows, tokens), bf16),
            pltpu.VMEM((ys - 1, rows, tokens), bf16),
            pltpu.VMEM((zs, strips, rows, LANES), f32),
            pltpu.VMEM((zs, strips, rows, LANES), bf16),
            pltpu.VMEM((zs, strips, rows, LANES), bf16),
            pltpu.VMEM((zs, strips, rows, LANES), bf16),
            pltpu.VMEM((depth * (depth + 1), 8, LANES), f32),
            pltpu.VMEM((3, 8, LANES), f32),
            pltpu.VMEM((3, 8, LANES), f32),
            pltpu.VMEM((xs + ys, 8, LANES), f32),
            pltpu.VMEM((rows, cols), f32),
            dma((2 * depth + 1,)),
            dma,
            dma((ys - 1,)),
            dma((xs,)),
            dma((max(xs - 1, 1),)),
            dma((tensor_size, ys, chunks)),
            dma((ys - 1,)),
            dma((ys - 1, strips)),
            dma((zs,)),
            dma((zs * (strips + chunks) + 2,)),
            dma((3,)),
            dma((3,)),
            dma((xs + ys,)),
            dma((xs + ys,)),
        ],
        compiler_params=pltpu.CompilerParams(
            collective_id=0, has_side_effects=True, vmem_limit_bytes=67000000
        ),
    )(layer_outs, avg_grads, attn_mixed, dwa_coefs)
    half = rows // 2
    return pl.pallas_call(
        settle,
        grid=(2,),
        out_shape=(
            jax.ShapeDtypeStruct(dwa_coefs.shape, f32),
            jax.ShapeDtypeStruct((rows, cols), f32),
        ),
        in_specs=[
            pl.BlockSpec((8, LANES), lambda i: (0, 0)),
            pl.BlockSpec((half, cols), lambda i: (i, 0)),
        ],
        out_specs=(
            pl.BlockSpec(dwa_coefs.shape, lambda i: (0, 0)),
            pl.BlockSpec((half, cols), lambda i: (i, 0)),
        ),
    )(coef, proj)


def solution(mesh):
    sizes = (mesh.shape["dp"], mesh.shape["tensor"])
    in_specs = (P(None, "dp", "tensor"), P(None, "dp", "tensor"), P("dp", "tensor"), P())
    out_specs = (P(), P("dp", "tensor"))
    return jax.shard_map(
        functools.partial(local, *sizes), mesh=mesh, in_specs=in_specs, out_specs=out_specs, check_vma=False
    )
```

```python
import functools

import jax
import jax.numpy as jnp
from jax import lax
from jax.experimental import pallas as pl
from jax.experimental.pallas import tpu as pltpu
from jax.sharding import PartitionSpec as P

LANES = 128
LAG = 1
SKEW = 2


def kernel(
    dp_size, tensor_size, outs_hbm, grads_hbm, attn_hbm, coefs, coef_out, proj_out,
    outs, grads, attn, gathered, g_send, own, z_send, z_left, z_right, sums_ref, coef_a, coef_b, coef_c, result,
    load_sem, attn_sem, gy_sem, p_sem, x_sem, g_recv, a_sem, a_recv,
    z_send_sem, z_sem, ca_send, ca_recv, cb_send, cb_recv,
):
    depth, tokens, features = grads.shape
    rows, cols = result.shape
    strips = cols // LANES
    chunks = rows // LANES
    early = max(chunks // 2, 1)
    ys = dp_size // tensor_size
    zs = tensor_size
    xs = tensor_size // 2
    dp, tensor = lax.axis_index("dp"), lax.axis_index("tensor")
    z, y = dp // ys, dp % ys
    x, core = tensor // 2, tensor % 2
    partner = x * 2 + 1 - core
    beside = jnp.where(z == 0, 1, jnp.where(z == zs - 1, zs - 2, -1))
    two = min(2, strips)
    mesh_id = pl.DeviceIdType.MESH

    loads = []
    for i in (depth - 2, depth - 1):
        loads.append(pltpu.make_async_copy(grads_hbm.at[i], grads.at[i], load_sem.at[i]))
    for i in range(depth - 2):
        loads.append(pltpu.make_async_copy(grads_hbm.at[i], grads.at[i], load_sem.at[i]))
    for j in range(depth + 1):
        loads.append(pltpu.make_async_copy(outs_hbm.at[j], outs.at[j], load_sem.at[depth + j]))
    mine = pl.ds(pl.multiple_of(y * tokens, tokens), tokens)
    attn_loads = [
        pltpu.make_async_copy(
            attn_hbm.at[:, pl.ds(k * LANES, LANES)], attn.at[k, mine, :], attn_sem
        )
        for k in range(strips)
    ]
    loads[0].start()
    loads[1].start()
    for load in attn_loads:
        load.start()
    for load in loads[2:]:
        load.start()

    barrier = pltpu.get_barrier_semaphore()

    def greet(**device):
        pl.semaphore_signal(barrier, inc=1, device_id=device, device_id_type=mesh_id)

    greet(tensor=partner)
    for i in range(1, ys):
        greet(dp=z * ys + (y + i) % ys)
    for n in range(1, xs):
        greet(tensor=(x + n) % xs * 2 + core)

    @pl.when(z > 0)
    def _():
        greet(dp=dp - ys)

    @pl.when(z < zs - 1)
    def _():
        greet(dp=dp + ys)

    def meet():
        ends = jnp.where(z == 0, 1, 0) + jnp.where(z == zs - 1, 1, 0)
        pl.semaphore_wait(barrier, 1 + (ys - 1) + (xs - 1) + 2 - ends)

    def lane_rows(c, count=1):
        return pl.ds(c * LANES, LANES * count)

    def piece(slot, part, c):
        return gathered.at[slot, part, lane_rows(c), :]

    def y_copy(i, c):
        return pltpu.make_async_remote_copy(
            src_ref=g_send.at[i - 1, lane_rows(c), :], dst_ref=piece(tensor, y, c),
            send_sem=gy_sem.at[i - 1], recv_sem=g_recv.at[tensor, y, c],
            device_id={"dp": z * ys + (y + i) % ys}, device_id_type=mesh_id,
        )

    def partner_copy(slot, part, c):
        return pltpu.make_async_remote_copy(
            src_ref=piece(slot, part, c), dst_ref=piece(slot, part, c),
            send_sem=p_sem.at[slot // 2], recv_sem=g_recv.at[slot, part, c],
            device_id={"tensor": partner}, device_id_type=mesh_id,
        )

    def x_copy(n, part, c):
        return pltpu.make_async_remote_copy(
            src_ref=piece(tensor, part, c), dst_ref=piece(tensor, part, c),
            send_sem=x_sem.at[n - 1], recv_sem=g_recv.at[tensor, part, c],
            device_id={"tensor": (x + n) % xs * 2 + core}, device_id_type=mesh_id,
        )

    def arrive(slot, part, c):
        partner_copy(slot, part, c).wait_recv()

    def attn_copy(i, k):
        return pltpu.make_async_remote_copy(
            src_ref=attn.at[k, mine, :], dst_ref=attn.at[k, mine, :],
            send_sem=a_sem.at[i - 1], recv_sem=a_recv.at[ys - i - 1, k],
            device_id={"dp": z * ys + (y + i) % ys}, device_id_type=mesh_id,
        )

    def attn_arrive(k):
        for i in range(1, ys):
            part = (y + i) % ys
            there = pl.ds(pl.multiple_of(part * tokens, tokens), tokens)
            pltpu.make_async_remote_copy(
                src_ref=attn.at[k, there, :], dst_ref=attn.at[k, there, :],
                send_sem=a_sem.at[i - 1], recv_sem=a_recv.at[i - 1, k],
                device_id={"dp": z * ys + part}, device_id_type=mesh_id,
            ).wait_recv()

    def make(part, c, into):
        first, second = coefs[depth - 2, depth - 1], coefs[depth - 1, depth - 1]

        @pl.loop(0, tokens // LANES)
        def _(step):
            at = pl.ds(pl.multiple_of(step * LANES, LANES), LANES)
            wide = pl.ds(pl.multiple_of(part * rows + c * LANES, LANES), LANES)
            value = first * grads[depth - 2, at, wide].astype(jnp.float32)
            value += second * grads[depth - 1, at, wide].astype(jnp.float32)
            into[lane_rows(c), at] = value.T.astype(jnp.bfloat16)

    def make_sent(c):
        for i in range(1, ys):
            make((y + i) % ys, c, g_send.at[i - 1])

    def make_own(c):
        make(y, c, gathered.at[tensor, y])
        partner_copy(tensor, y, c).start()

    def send_y(c):
        for i in range(1, ys):
            y_copy(i, c).start()

    def send_x(part, c):
        for n in range(1, xs):
            x_copy(n, part, c).start()

    def send_attn(k_first, k_end):
        for k in range(k_first, k_end):
            for i in range(1, ys):
                attn_copy(i, k).start()

    def relay_y(c):
        for i in range(1, ys):
            part = (y + i) % ys
            arrive(tensor, part, c)
            partner_copy(tensor, part, c).start()
            send_x(part, c)

    others = [((x + n) % xs) * 2 for n in range(1, xs)]

    def relay_x(part, c, when):
        for other in others:
            @pl.when(when(other + core))
            def _():
                arrive(other + core, part, c)
                partner_copy(other + core, part, c).start()

    messages = [(0, early, k, k + 1) for k in range(strips)]
    halves = [(0, strips // 2), (strips // 2, strips)] if strips > 1 else [(0, strips)]
    rest = chunks - early
    late = [(c, 1) + half for c in range(early, chunks) for half in halves]
    soon = [(early, rest, 0, two)] + [(early, rest, k, k + 1) for k in range(two, strips)] if rest else []
    late_ids = range(strips, strips + len(late))
    soon_ids = range(strips + len(late), strips + len(late) + len(soon))
    messages = messages + late + soon

    def window(m):
        c, count, k_first, k_end = messages[m]
        return pl.ds(k_first, k_end - k_first), pl.ds(c * LANES, LANES * count)

    passing = strips + len(late)

    def arrival(slot, m):
        return slot * passing + m

    def right_copy(slot, m, sem):
        ks, at = window(m)
        return pltpu.make_async_remote_copy(
            src_ref=z_send.at[slot, ks, at, :], dst_ref=z_left.at[slot, ks, at, :],
            send_sem=z_send_sem.at[slot], recv_sem=z_sem.at[sem],
            device_id={"dp": dp + ys}, device_id_type=mesh_id,
        )

    def left_copy(slot, m, sem):
        ks, at = window(m)
        return pltpu.make_async_remote_copy(
            src_ref=z_send.at[slot, ks, at, :], dst_ref=z_right.at[slot, ks, at, :],
            send_sem=z_send_sem.at[slot], recv_sem=z_sem.at[sem],
            device_id={"dp": dp - ys}, device_id_type=mesh_id,
        )

    def send_right(slot, m):
        sem = zs * passing if m in soon_ids else jnp.where(slot == z + 1, zs * passing, arrival(slot, m))
        right_copy(slot, m, sem).start()

    def send_left(slot, m):
        sem = zs * passing + 1 if m in soon_ids else jnp.where(slot == z - 1, zs * passing + 1, arrival(slot, m))
        left_copy(slot, m, sem).start()

    def product(slot, k, c, count, width=1):
        at = pl.ds(c * LANES, LANES * count)
        left = jnp.concatenate([gathered[slot, part, at, :] for part in range(ys)], axis=1)
        right = jnp.concatenate([attn[k + n] for n in range(width)], axis=1)
        value = jnp.dot(left, right, preferred_element_type=jnp.float32)
        return [value[:, n * LANES : (n + 1) * LANES] for n in range(width)]

    def compute(slot, m):
        c, count, k_first, k_end = messages[m]
        at = pl.ds(c * LANES, LANES * count)
        rightmost, leftmost = (slot > z) & (z == 0), (slot < z) & (z == zs - 1)

        width = 2 - (k_end - k_first) % 2

        @pl.loop(k_first, k_end, step=width)
        def _(k):
            values = product(slot, k, c, count, width)

            @pl.when(rightmost | leftmost)
            def _():
                for n, value in enumerate(values):
                    z_send[slot, k + n, at, :] = value.astype(jnp.bfloat16)

            @pl.when(jnp.logical_not(rightmost | leftmost))
            def _():
                for n, value in enumerate(values):
                    own[slot, k + n, at, :] = value

        @pl.when(rightmost)
        def _():
            send_right(slot, m)

        @pl.when(leftmost)
        def _():
            send_left(slot, m)

    def pass_on(slot, m, hop):
        c, count, k_first, k_end = messages[m]
        at = pl.ds(c * LANES, LANES * count)

        @pl.when((slot > z) & (z == hop))
        def _():
            right_copy(slot, m, arrival(slot, m)).wait_recv()
            for k in range(k_first, k_end):
                value = own[slot, k, at, :] + z_left[slot, k, at, :].astype(jnp.float32)
                z_send[slot, k, at, :] = value.astype(jnp.bfloat16)
            send_right(slot, m)

        @pl.when((slot < z) & (z == zs - 1 - hop))
        def _():
            left_copy(slot, m, arrival(slot, m)).wait_recv()
            for k in range(k_first, k_end):
                value = own[slot, k, at, :] + z_right[slot, k, at, :].astype(jnp.float32)
                z_send[slot, k, at, :] = value.astype(jnp.bfloat16)
            send_left(slot, m)

    pairs = [(i, j) for i in range(depth) for j in range(min(i + 2, depth + 1))]
    quarters = 4

    def coef_partial(quarter):
        size = tokens // 16 // quarters

        def step(r, sums):
            at = pl.ds(pl.multiple_of(r * 16, 16), 16)
            sums = list(sums)
            for col in range(features // LANES):
                lanes = slice(col * LANES, (col + 1) * LANES)
                g = [grads[i, at, lanes].astype(jnp.float32) for i in range(depth)]
                o = [outs[j, at, lanes].astype(jnp.float32) for j in range(depth + 1)]
                for n, (i, j) in enumerate(pairs):
                    value = g[i] * o[j]
                    sums[n] += value[:8] + value[8:]
            return tuple(sums)

        zero = jnp.zeros((8, LANES), jnp.float32)
        first = tuple(zero if quarter == 0 else sums_ref[n] for n in range(len(pairs)))
        sums = lax.fori_loop(quarter * size, (quarter + 1) * size, step, first)
        for n in range(len(pairs)):
            sums_ref[n] = sums[n]

    def coef_tile():
        row = lax.broadcasted_iota(jnp.int32, (8, LANES), 0)
        col = lax.broadcasted_iota(jnp.int32, (8, LANES), 1)
        tile = jnp.zeros((8, LANES), jnp.float32)
        for n, (i, j) in enumerate(pairs):
            value = jnp.sum(sums_ref[n], axis=(0, 1), keepdims=True)
            tile = jnp.where((row == i) & (col == j), value, tile)
        return tile

    def coef_hop(stage, target):
        return pltpu.make_async_remote_copy(
            src_ref=coef_a.at[stage], dst_ref=coef_b.at[stage],
            send_sem=ca_send.at[stage], recv_sem=ca_recv.at[stage],
            device_id=target, device_id_type=mesh_id,
        )

    def coef_step(step):
        if step < zs:
            @pl.when(z == step)
            def _():
                coef_a[0] = coef_tile()
                if step > 0:
                    coef_hop(0, {"dp": dp + ys}).wait_recv()
                    coef_a[0] += coef_b[0]
                if step < zs - 1:
                    coef_hop(0, {"dp": dp + ys}).start()
                else:
                    coef_a[1] = coef_a[0]
                    coef_hop(1, {"dp": dp - ys}).start()
        else:
            plane = 2 * zs - 2 - step

            @pl.when(z == plane)
            def _():
                coef_hop(1, {"dp": dp - ys}).wait_recv()
                coef_a[1] = coef_b[1]
                if plane > 0:
                    coef_hop(1, {"dp": dp - ys}).start()

    def coef_partner(start):
        if start:
            coef_hop(2, {"tensor": partner}).start()
        else:
            coef_hop(2, {"tensor": partner}).wait_recv()

    def coef_x(n, at):
        return pltpu.make_async_remote_copy(
            src_ref=coef_c.at[at], dst_ref=coef_c.at[at],
            send_sem=cb_send.at[n], recv_sem=cb_recv.at[at],
            device_id={"tensor": (x + n) % xs * 2 + core}, device_id_type=mesh_id,
        )

    def coef_y(i, at):
        return pltpu.make_async_remote_copy(
            src_ref=coef_c.at[xs + at], dst_ref=coef_c.at[xs + at],
            send_sem=cb_send.at[xs + i], recv_sem=cb_recv.at[xs + at],
            device_id={"dp": z * ys + (y + i) % ys}, device_id_type=mesh_id,
        )

    last = tensor == z
    first = tensor == beside
    plain = jnp.logical_not(last | first)
    sooner = jnp.logical_not(last)
    parts = [y] + [(y + i) % ys for i in range(1, ys)]

    def away(slot):
        return slot != z

    def home(slot):
        return slot == z

    def never(slot):
        return slot < 0

    def near(slot):
        return (slot != z) & (slot // 2 == x)

    def far(slot):
        return (slot != z) & (slot // 2 != x)

    def outer(slot):
        return far(slot) & ((slot == 0) | (slot == zs - 1))

    def inner(slot):
        return far(slot) & (slot != 0) & (slot != zs - 1)

    def is_first(slot):
        return slot == beside

    def is_plain(slot):
        return (slot != z) & (slot != beside)

    def near_plain(slot):
        return near(slot) & (slot != beside)

    def far_plain(slot):
        return far(slot) & (slot != beside)

    def near_first(slot):
        return (slot == beside) & (slot // 2 == x)

    def far_first(slot):
        return (slot == beside) & (slot // 2 != x)

    def slot_at(i):
        outer = jnp.where(i % 2 == 0, zs - 1 - i // 2, i // 2)
        return jnp.where(z < zs // 2, outer, zs - 1 - outer)

    def late_of(c):
        return late_ids[(c - early) * len(halves) : (c - early + 1) * len(halves)]

    queue, done = [], {hop: 0 for hop in range(1, zs - 1)}

    def advance(hop, limit):
        while hop in done and done[hop] < min(limit, len(queue)):
            follow(*queue[done[hop]], hop)
            done[hop] += 1

    def tick():
        for hop in done:
            advance(hop, len(queue) - LAG - (hop - 1) * SKEW)

    def flush():
        while any(place < len(queue) for place in done.values()):
            for hop in done:
                ahead = done.get(hop - 1, len(queue))
                limit = ahead if ahead == len(queue) else ahead - 1
                advance(hop, min(done[hop] + hop, limit))

    def follow(ms, passed, hop):
        @pl.loop(0, zs)
        def _(i):
            slot = slot_at(i)

            @pl.when(passed(slot))
            def _():
                for m in ms:
                    pass_on(slot, m, hop)

    def run(ms, when, passed):
        @pl.loop(0, zs)
        def _(i):
            slot = slot_at(i)

            @pl.when(when(slot))
            def _():
                for m in ms:
                    compute(slot, m)

        if passed is not never:
            queue.append((ms, passed))

    def gather_partner(slot, c_first, c_end, when):
        @pl.when(when(slot))
        def _():
            for c in range(c_first, c_end):
                for part in parts:
                    arrive(slot, part, c)

    steps = list(range(2 * zs - 1))
    share = -(-len(steps) // 7)

    def coef_steps():
        for step in steps[:share]:
            coef_step(step)
        del steps[:share]

    loads[0].wait()
    loads[1].wait()
    make_sent(0)
    meet()

    @pl.when(sooner)
    def _():
        send_y(0)

    make_own(0)

    @pl.when(sooner)
    def _():
        send_x(y, 0)

    for c in range(1, early):
        make_sent(c)

        @pl.when(sooner)
        def _():
            send_y(c)

    pltpu.make_async_copy(attn.at[:, mine, :], attn.at[:, mine, :], attn_sem).wait()
    send_attn(0, two)

    @pl.when(first)
    def _():
        for c in range(early, chunks):
            make_sent(c)
            send_y(c)

    send_attn(two, strips - rest)

    @pl.when(jnp.logical_not(plain))
    def _():
        send_attn(strips - rest, strips)

    for c in range(1, early):
        make_own(c)
    for load in loads[2:]:
        load.wait()

    coef_partial(0)
    for c in range(early):
        @pl.when(sooner)
        def _():
            relay_y(c)
            if c + 1 < early:
                send_x(y, c + 1)

        if c == 0:
            relay_x(y, 0, away)
        coef_partial(1 + c if early > 1 else 1)
    for quarter in range(1 + max(early, 1), quarters):
        coef_partial(quarter)
    coef_steps()
    for part in parts[1:]:
        relay_x(part, 0, away)

    @pl.when(first)
    def _():
        for c in range(early, chunks):
            make_own(c)
            send_x(y, c)

    attn_arrive(0)
    gather_partner(partner, 0, early, away)
    run([0], near, near)
    tick()
    coef_steps()
    for c in range(1, early):
        relay_x(y, c, away)
    coef_steps()
    if two > 1:
        attn_arrive(1)
        run([1], near, near)
        tick()
    coef_steps()
    for c in range(1, early):
        for part in parts[1:]:
            relay_x(part, c, away)
    catch = min(two + 2, strips - 1)
    for other in others:
        gather_partner(other + 1 - core, 0, early, away)
    for k in range(two):
        run([k], far, far)
        tick()
    if rest:
        @pl.when(plain | last)
        def _():
            for c in range(early, chunks):
                make_sent(c)

        @pl.when(plain)
        def _():
            for n in range(rest):
                send_y(early + n)
                send_attn(strips - rest + n, strips - rest + n + 1)

        @pl.when(plain | last)
        def _():
            for c in range(early, chunks):
                make_own(c)

        @pl.when(plain)
        def _():
            for c in range(early, chunks):
                send_x(y, c)

    @pl.when(last)
    def _():
        for c in range(chunks):
            send_y(c)

    def late_near(c, ms):
        @pl.when(plain)
        def _():
            relay_y(c)

        relay_x(y, c, is_plain)
        gather_partner(partner, c, c + 1, is_plain)
        run(ms, near_plain, near)

    def late_far(c):
        for part in parts[1:]:
            relay_x(part, c, is_plain)
        for other in others:
            gather_partner(other + 1 - core, c, c + 1, is_plain)

    for k in range(two, strips):
        n = k - (strips - rest)
        if n >= 0:
            late_near(early + n, late_of(early + n)[:1])
        if n == 1:
            late_far(early)
            run(late_of(early)[:1], far_plain, far)
        if k == two and rest:
            @pl.when(first)
            def _():
                for c in range(early, chunks):
                    relay_y(c)

        attn_arrive(k)
        run([k], away, away)
        tick()
        if rest:
            have = soon_ids[: k - two + 2]
            if k == two:
                gather_partner(partner, early, chunks, is_first)
            run(have if k == two else have[-1:], near_first, never)
            if k == catch:
                for c in range(early, chunks):
                    for part in parts:
                        relay_x(part, c, is_first)
                for other in others:
                    gather_partner(other + 1 - core, early, chunks, is_first)
            if k >= catch:
                run(have if k == catch else have[-1:], far_first, never)
        if k % 2:
            coef_steps()
        if k == two:
            @pl.when(last)
            def _():
                for c in range(chunks):
                    send_x(y, c)
    while steps:
        coef_steps()
    coef_a[2] = coef_a[1]
    coef_partner(True)

    for c in range(chunks):
        relay_x(y, c, home)
    started = len(queue)

    @pl.when(last)
    def _():
        for c in range(chunks // 2):
            relay_y(c)

    if rest:
        run([m for c in range(early, chunks) for m in late_of(c)[1:]], near_plain, near)
        advance(1, started)

    @pl.when(last)
    def _():
        for c in range(chunks // 2, chunks):
            relay_y(c)

    advance(2, started - 1)
    coef_partner(False)
    coef_c[x] = coef_a[2] + coef_b[2]
    for n in range(1, xs):
        coef_x(n, x).start()
    if rest:
        left = list(late_of(early)[1:])
        for c in range(early + 1, chunks):
            late_far(c)
            left += late_of(c)
        run(left, far_plain, outer)
        queue.append((left, inner))
        advance(1, len(queue))
    for n in range(1, xs):
        coef_x(n, (x + n) % xs).wait_recv()
    total = coef_c[0]
    for n in range(1, xs):
        total += coef_c[n]
    coef_c[xs + y] = total
    for i in range(1, ys):
        coef_y(i, y).start()

    for c in range(chunks):
        for part in parts[1:]:
            relay_x(part, c, home)
    flush()

    @pl.when(z % 2 != core)
    def _():
        for c in range(chunks):
            for part in parts:
                arrive(z, part, c)

    width = 2 - strips % 2

    @pl.loop(0, strips, step=width)
    def _(k):
        for n, value in enumerate(product(z, k, 0, chunks, width)):
            own[z, k + n] = value

    for i in range(1, ys):
        coef_y(i, (y + i) % ys).wait_recv()
    total = coef_c[xs]
    for i in range(1, ys):
        total += coef_c[xs + i]
    coef_b[2] = total
    coef_store = pltpu.make_async_copy(coef_b.at[2], coef_out, load_sem.at[0])
    coef_store.start()

    @pl.when(z > 0)
    def _():
        pltpu.make_async_remote_copy(
            src_ref=z_left.at[z], dst_ref=z_left.at[z],
            send_sem=z_send_sem.at[z], recv_sem=z_sem.at[zs * passing],
            device_id={"dp": dp - ys}, device_id_type=mesh_id,
        ).wait_recv()

    @pl.when(z < zs - 1)
    def _():
        pltpu.make_async_remote_copy(
            src_ref=z_right.at[z], dst_ref=z_right.at[z],
            send_sem=z_send_sem.at[z], recv_sem=z_sem.at[zs * passing + 1],
            device_id={"dp": dp + ys}, device_id_type=mesh_id,
        ).wait_recv()

    for c in range(chunks):
        at = lane_rows(c)
        for k in range(strips):
            lanes = slice(k * LANES, (k + 1) * LANES)
            result[at, lanes] = own[z, k, at, :]

            @pl.when(z > 0)
            def _():
                result[at, lanes] += z_left[z, k, at, :].astype(jnp.float32)

            @pl.when(z < zs - 1)
            def _():
                result[at, lanes] += z_right[z, k, at, :].astype(jnp.float32)

        pltpu.make_async_copy(result.at[at, :], proj_out.at[at, :], attn_sem).start()

    @pl.loop(0, zs)
    def _(slot):
        @pl.when(slot != z)
        def _():
            pltpu.make_async_remote_copy(
                src_ref=z_send.at[slot], dst_ref=z_left.at[slot],
                send_sem=z_send_sem.at[slot], recv_sem=z_sem.at[0],
                device_id={"dp": z * ys + (y + 1) % ys}, device_id_type=mesh_id,
            ).wait_send()

    def sent(ref, sem):
        pltpu.make_async_remote_copy(
            src_ref=ref, dst_ref=ref, send_sem=sem, recv_sem=z_sem.at[0],
            device_id={"tensor": partner}, device_id_type=mesh_id,
        ).wait_send()

    for i in range(1, ys):
        sent(g_send.at[i - 1], gy_sem.at[i - 1])
        sent(attn.at[:, mine, :], a_sem.at[i - 1])
    for n in range(xs):
        sent(gathered.at[n * 2 + core], p_sem.at[n])
    for n in range(1, xs):
        sent(gathered.at[tensor], x_sem.at[n - 1])

    @pl.when(z < zs - 1)
    def _():
        coef_hop(0, {"dp": dp + ys}).wait_send()

    @pl.when(z > 0)
    def _():
        coef_hop(1, {"dp": dp - ys}).wait_send()

    coef_hop(2, {"tensor": partner}).wait_send()
    for n in range(1, xs):
        coef_x(n, x).wait_send()
    for i in range(1, ys):
        coef_y(i, y).wait_send()
    coef_store.wait()
    pltpu.make_async_copy(result, proj_out, attn_sem).wait()


def settle(coef, proj, coef_out, proj_out):
    coef_out[...] = coef[: coef_out.shape[0], : coef_out.shape[1]]
    proj_out[...] = proj[...]


def local(dp_size, tensor_size, layer_outs, avg_grads, attn_mixed, dwa_coefs):
    depth, tokens, features = avg_grads.shape
    rows = features * tensor_size // dp_size
    cols = attn_mixed.shape[1]
    ys, zs, xs = dp_size // tensor_size, tensor_size, tensor_size // 2
    strips, chunks = cols // LANES, rows // LANES
    bf16, f32 = jnp.bfloat16, jnp.float32
    dma = pltpu.SemaphoreType.DMA
    any_space = pl.BlockSpec(memory_space=pl.ANY)
    coef, proj = pl.pallas_call(
        functools.partial(kernel, dp_size, tensor_size),
        out_shape=(
            jax.ShapeDtypeStruct((8, LANES), f32),
            jax.ShapeDtypeStruct((rows, cols), f32),
        ),
        in_specs=[any_space, any_space, any_space, pl.BlockSpec(memory_space=pltpu.SMEM)],
        out_specs=(any_space, any_space),
        scratch_shapes=[
            pltpu.VMEM(layer_outs.shape, bf16),
            pltpu.VMEM(avg_grads.shape, bf16),
            pltpu.VMEM((strips, ys * tokens, LANES), bf16),
            pltpu.VMEM((zs, ys, rows, tokens), bf16),
            pltpu.VMEM((ys - 1, rows, tokens), bf16),
            pltpu.VMEM((zs, strips, rows, LANES), f32),
            pltpu.VMEM((zs, strips, rows, LANES), bf16),
            pltpu.VMEM((zs, strips, rows, LANES), bf16),
            pltpu.VMEM((zs, strips, rows, LANES), bf16),
            pltpu.VMEM((depth * (depth + 1), 8, LANES), f32),
            pltpu.VMEM((3, 8, LANES), f32),
            pltpu.VMEM((3, 8, LANES), f32),
            pltpu.VMEM((xs + ys, 8, LANES), f32),
            pltpu.VMEM((rows, cols), f32),
            dma((2 * depth + 1,)),
            dma,
            dma((ys - 1,)),
            dma((xs,)),
            dma((max(xs - 1, 1),)),
            dma((tensor_size, ys, chunks)),
            dma((ys - 1,)),
            dma((ys - 1, strips)),
            dma((zs,)),
            dma((zs * (strips + chunks) + 2,)),
            dma((3,)),
            dma((3,)),
            dma((xs + ys,)),
            dma((xs + ys,)),
        ],
        compiler_params=pltpu.CompilerParams(
            collective_id=0, has_side_effects=True, vmem_limit_bytes=67000000
        ),
    )(layer_outs, avg_grads, attn_mixed, dwa_coefs)
    half = rows // 2
    return pl.pallas_call(
        settle,
        grid=(2,),
        out_shape=(
            jax.ShapeDtypeStruct(dwa_coefs.shape, f32),
            jax.ShapeDtypeStruct((rows, cols), f32),
        ),
        in_specs=[
            pl.BlockSpec((8, LANES), lambda i: (0, 0)),
            pl.BlockSpec((half, cols), lambda i: (i, 0)),
        ],
        out_specs=(
            pl.BlockSpec(dwa_coefs.shape, lambda i: (0, 0)),
            pl.BlockSpec((half, cols), lambda i: (i, 0)),
        ),
    )(coef, proj)


def solution(mesh):
    sizes = (mesh.shape["dp"], mesh.shape["tensor"])
    in_specs = (P(None, "dp", "tensor"), P(None, "dp", "tensor"), P("dp", "tensor"), P())
    out_specs = (P(), P("dp", "tensor"))
    return jax.shard_map(
        functools.partial(local, *sizes), mesh=mesh, in_specs=in_specs, out_specs=out_specs, check_vma=False
    )
```

```python
import functools

import jax
import jax.numpy as jnp
from jax import lax
from jax.experimental import pallas as pl
from jax.experimental.pallas import tpu as pltpu
from jax.sharding import PartitionSpec as P

LANES = 128
LAG = 1
SKEW = 2


def kernel(
    dp_size, tensor_size, outs_hbm, grads_hbm, attn_hbm, coefs, coef_out, proj_out,
    outs, grads, attn, gathered, g_send, own, z_send, z_left, z_right, sums_ref, coef_a, coef_b, coef_c, result,
    load_sem, attn_sem, gy_sem, p_sem, x_sem, g_recv, a_sem, a_recv,
    z_send_sem, z_sem, ca_send, ca_recv, cb_send, cb_recv,
):
    depth, tokens, features = grads.shape
    rows, cols = result.shape
    strips = cols // LANES
    chunks = rows // LANES
    early = max(chunks // 2, 1)
    ys = dp_size // tensor_size
    zs = tensor_size
    xs = tensor_size // 2
    dp, tensor = lax.axis_index("dp"), lax.axis_index("tensor")
    z, y = dp // ys, dp % ys
    x, core = tensor // 2, tensor % 2
    partner = x * 2 + 1 - core
    beside = jnp.where(z == 0, 1, jnp.where(z == zs - 1, zs - 2, -1))
    two = min(2, strips)
    mesh_id = pl.DeviceIdType.MESH

    loads = []
    for i in (depth - 2, depth - 1):
        loads.append(pltpu.make_async_copy(grads_hbm.at[i], grads.at[i], load_sem.at[i]))
    for i in range(depth - 2):
        loads.append(pltpu.make_async_copy(grads_hbm.at[i], grads.at[i], load_sem.at[i]))
    for j in range(depth + 1):
        loads.append(pltpu.make_async_copy(outs_hbm.at[j], outs.at[j], load_sem.at[depth + j]))
    mine = pl.ds(pl.multiple_of(y * tokens, tokens), tokens)
    attn_loads = [
        pltpu.make_async_copy(
            attn_hbm.at[:, pl.ds(k * LANES, LANES)], attn.at[k, mine, :], attn_sem
        )
        for k in range(strips)
    ]
    loads[0].start()
    loads[1].start()
    for load in attn_loads:
        load.start()
    for load in loads[2:]:
        load.start()

    barrier = pltpu.get_barrier_semaphore()

    def greet(**device):
        pl.semaphore_signal(barrier, inc=1, device_id=device, device_id_type=mesh_id)

    greet(tensor=partner)
    for i in range(1, ys):
        greet(dp=z * ys + (y + i) % ys)
    for n in range(1, xs):
        greet(tensor=(x + n) % xs * 2 + core)

    @pl.when(z > 0)
    def _():
        greet(dp=dp - ys)

    @pl.when(z < zs - 1)
    def _():
        greet(dp=dp + ys)

    def meet():
        ends = jnp.where(z == 0, 1, 0) + jnp.where(z == zs - 1, 1, 0)
        pl.semaphore_wait(barrier, 1 + (ys - 1) + (xs - 1) + 2 - ends)

    def lane_rows(c, count=1):
        return pl.ds(c * LANES, LANES * count)

    def piece(slot, part, c):
        return gathered.at[slot, part, lane_rows(c), :]

    def y_copy(i, c):
        return pltpu.make_async_remote_copy(
            src_ref=g_send.at[i - 1, lane_rows(c), :], dst_ref=piece(tensor, y, c),
            send_sem=gy_sem.at[i - 1], recv_sem=g_recv.at[tensor, y, c],
            device_id={"dp": z * ys + (y + i) % ys}, device_id_type=mesh_id,
        )

    def partner_copy(slot, part, c):
        return pltpu.make_async_remote_copy(
            src_ref=piece(slot, part, c), dst_ref=piece(slot, part, c),
            send_sem=p_sem.at[slot // 2], recv_sem=g_recv.at[slot, part, c],
            device_id={"tensor": partner}, device_id_type=mesh_id,
        )

    def x_copy(n, part, c):
        return pltpu.make_async_remote_copy(
            src_ref=piece(tensor, part, c), dst_ref=piece(tensor, part, c),
            send_sem=x_sem.at[n - 1], recv_sem=g_recv.at[tensor, part, c],
            device_id={"tensor": (x + n) % xs * 2 + core}, device_id_type=mesh_id,
        )

    def arrive(slot, part, c):
        partner_copy(slot, part, c).wait_recv()

    def attn_copy(i, k):
        return pltpu.make_async_remote_copy(
            src_ref=attn.at[k, mine, :], dst_ref=attn.at[k, mine, :],
            send_sem=a_sem.at[i - 1], recv_sem=a_recv.at[ys - i - 1, k],
            device_id={"dp": z * ys + (y + i) % ys}, device_id_type=mesh_id,
        )

    def attn_arrive(k):
        for i in range(1, ys):
            part = (y + i) % ys
            there = pl.ds(pl.multiple_of(part * tokens, tokens), tokens)
            pltpu.make_async_remote_copy(
                src_ref=attn.at[k, there, :], dst_ref=attn.at[k, there, :],
                send_sem=a_sem.at[i - 1], recv_sem=a_recv.at[i - 1, k],
                device_id={"dp": z * ys + part}, device_id_type=mesh_id,
            ).wait_recv()

    def make(part, c, into):
        first, second = coefs[depth - 2, depth - 1], coefs[depth - 1, depth - 1]

        @pl.loop(0, tokens // LANES)
        def _(step):
            at = pl.ds(pl.multiple_of(step * LANES, LANES), LANES)
            wide = pl.ds(pl.multiple_of(part * rows + c * LANES, LANES), LANES)
            value = first * grads[depth - 2, at, wide].astype(jnp.float32)
            value += second * grads[depth - 1, at, wide].astype(jnp.float32)
            into[lane_rows(c), at] = value.T.astype(jnp.bfloat16)

    def make_sent(c):
        for i in range(1, ys):
            make((y + i) % ys, c, g_send.at[i - 1])

    def make_own(c):
        make(y, c, gathered.at[tensor, y])
        partner_copy(tensor, y, c).start()

    def send_y(c):
        for i in range(1, ys):
            y_copy(i, c).start()

    def send_x(part, c):
        for n in range(1, xs):
            x_copy(n, part, c).start()

    def send_attn(k_first, k_end):
        for k in range(k_first, k_end):
            for i in range(1, ys):
                attn_copy(i, k).start()

    def relay_y(c):
        for i in range(1, ys):
            part = (y + i) % ys
            arrive(tensor, part, c)
            partner_copy(tensor, part, c).start()
            send_x(part, c)

    others = [((x + n) % xs) * 2 for n in range(1, xs)]

    def relay_x(part, c, when):
        for other in others:
            @pl.when(when(other + core))
            def _():
                arrive(other + core, part, c)
                partner_copy(other + core, part, c).start()

    messages = [(0, early, k, k + 1) for k in range(strips)]
    halves = [(0, strips // 2), (strips // 2, strips)] if strips > 1 else [(0, strips)]
    rest = chunks - early
    late = [(c, 1) + half for c in range(early, chunks) for half in halves]
    soon = [(early, rest, 0, two)] + [(early, rest, k, k + 1) for k in range(two, strips)] if rest else []
    late_ids = range(strips, strips + len(late))
    soon_ids = range(strips + len(late), strips + len(late) + len(soon))
    messages = messages + late + soon

    def window(m):
        c, count, k_first, k_end = messages[m]
        return pl.ds(k_first, k_end - k_first), pl.ds(c * LANES, LANES * count)

    passing = strips + len(late)

    def arrival(slot, m):
        return slot * passing + m

    def right_copy(slot, m, sem):
        ks, at = window(m)
        return pltpu.make_async_remote_copy(
            src_ref=z_send.at[slot, ks, at, :], dst_ref=z_left.at[slot, ks, at, :],
            send_sem=z_send_sem.at[slot], recv_sem=z_sem.at[sem],
            device_id={"dp": dp + ys}, device_id_type=mesh_id,
        )

    def left_copy(slot, m, sem):
        ks, at = window(m)
        return pltpu.make_async_remote_copy(
            src_ref=z_send.at[slot, ks, at, :], dst_ref=z_right.at[slot, ks, at, :],
            send_sem=z_send_sem.at[slot], recv_sem=z_sem.at[sem],
            device_id={"dp": dp - ys}, device_id_type=mesh_id,
        )

    def send_right(slot, m):
        sem = zs * passing if m in soon_ids else jnp.where(slot == z + 1, zs * passing, arrival(slot, m))
        right_copy(slot, m, sem).start()

    def send_left(slot, m):
        sem = zs * passing + 1 if m in soon_ids else jnp.where(slot == z - 1, zs * passing + 1, arrival(slot, m))
        left_copy(slot, m, sem).start()

    def product(slot, k, c, count, width=1):
        at = pl.ds(c * LANES, LANES * count)
        left = jnp.concatenate([gathered[slot, part, at, :] for part in range(ys)], axis=1)
        right = jnp.concatenate([attn[k + n] for n in range(width)], axis=1)
        value = jnp.dot(left, right, preferred_element_type=jnp.float32)
        return [value[:, n * LANES : (n + 1) * LANES] for n in range(width)]

    def compute(slot, m):
        c, count, k_first, k_end = messages[m]
        at = pl.ds(c * LANES, LANES * count)
        rightmost, leftmost = (slot > z) & (z == 0), (slot < z) & (z == zs - 1)

        width = 2 - (k_end - k_first) % 2

        @pl.loop(k_first, k_end, step=width)
        def _(k):
            values = product(slot, k, c, count, width)

            @pl.when(rightmost | leftmost)
            def _():
                for n, value in enumerate(values):
                    z_send[slot, k + n, at, :] = value.astype(jnp.bfloat16)

            @pl.when(jnp.logical_not(rightmost | leftmost))
            def _():
                for n, value in enumerate(values):
                    own[slot, k + n, at, :] = value

        @pl.when(rightmost)
        def _():
            send_right(slot, m)

        @pl.when(leftmost)
        def _():
            send_left(slot, m)

    def pass_on(slot, m, hop):
        c, count, k_first, k_end = messages[m]
        at = pl.ds(c * LANES, LANES * count)

        @pl.when((slot > z) & (z == hop))
        def _():
            right_copy(slot, m, arrival(slot, m)).wait_recv()
            for k in range(k_first, k_end):
                value = own[slot, k, at, :] + z_left[slot, k, at, :].astype(jnp.float32)
                z_send[slot, k, at, :] = value.astype(jnp.bfloat16)
            send_right(slot, m)

        @pl.when((slot < z) & (z == zs - 1 - hop))
        def _():
            left_copy(slot, m, arrival(slot, m)).wait_recv()
            for k in range(k_first, k_end):
                value = own[slot, k, at, :] + z_right[slot, k, at, :].astype(jnp.float32)
                z_send[slot, k, at, :] = value.astype(jnp.bfloat16)
            send_left(slot, m)

    pairs = [(i, j) for i in range(depth) for j in range(min(i + 2, depth + 1))]
    quarters = 4

    def coef_partial(quarter):
        size = tokens // 16 // quarters

        def step(r, sums):
            at = pl.ds(pl.multiple_of(r * 16, 16), 16)
            sums = list(sums)
            for col in range(features // LANES):
                lanes = slice(col * LANES, (col + 1) * LANES)
                g = [grads[i, at, lanes].astype(jnp.float32) for i in range(depth)]
                o = [outs[j, at, lanes].astype(jnp.float32) for j in range(depth + 1)]
                for n, (i, j) in enumerate(pairs):
                    value = g[i] * o[j]
                    sums[n] += value[:8] + value[8:]
            return tuple(sums)

        zero = jnp.zeros((8, LANES), jnp.float32)
        first = tuple(zero if quarter == 0 else sums_ref[n] for n in range(len(pairs)))
        sums = lax.fori_loop(quarter * size, (quarter + 1) * size, step, first)
        for n in range(len(pairs)):
            sums_ref[n] = sums[n]

    def coef_tile():
        row = lax.broadcasted_iota(jnp.int32, (8, LANES), 0)
        col = lax.broadcasted_iota(jnp.int32, (8, LANES), 1)
        tile = jnp.zeros((8, LANES), jnp.float32)
        for n, (i, j) in enumerate(pairs):
            value = jnp.sum(sums_ref[n], axis=(0, 1), keepdims=True)
            tile = jnp.where((row == i) & (col == j), value, tile)
        return tile

    def coef_hop(stage, target):
        return pltpu.make_async_remote_copy(
            src_ref=coef_a.at[stage], dst_ref=coef_b.at[stage],
            send_sem=ca_send.at[stage], recv_sem=ca_recv.at[stage],
            device_id=target, device_id_type=mesh_id,
        )

    def coef_step(step):
        if step < zs:
            @pl.when(z == step)
            def _():
                coef_a[0] = coef_tile()
                if step > 0:
                    coef_hop(0, {"dp": dp + ys}).wait_recv()
                    coef_a[0] += coef_b[0]
                if step < zs - 1:
                    coef_hop(0, {"dp": dp + ys}).start()
                else:
                    coef_a[1] = coef_a[0]
                    coef_hop(1, {"dp": dp - ys}).start()
        else:
            plane = 2 * zs - 2 - step

            @pl.when(z == plane)
            def _():
                coef_hop(1, {"dp": dp - ys}).wait_recv()
                coef_a[1] = coef_b[1]
                if plane > 0:
                    coef_hop(1, {"dp": dp - ys}).start()

    def coef_partner(start):
        if start:
            coef_hop(2, {"tensor": partner}).start()
        else:
            coef_hop(2, {"tensor": partner}).wait_recv()

    def coef_x(n, at):
        return pltpu.make_async_remote_copy(
            src_ref=coef_c.at[at], dst_ref=coef_c.at[at],
            send_sem=cb_send.at[n], recv_sem=cb_recv.at[at],
            device_id={"tensor": (x + n) % xs * 2 + core}, device_id_type=mesh_id,
        )

    def coef_y(i, at):
        return pltpu.make_async_remote_copy(
            src_ref=coef_c.at[xs + at], dst_ref=coef_c.at[xs + at],
            send_sem=cb_send.at[xs + i], recv_sem=cb_recv.at[xs + at],
            device_id={"dp": z * ys + (y + i) % ys}, device_id_type=mesh_id,
        )

    last = tensor == z
    first = tensor == beside
    plain = jnp.logical_not(last | first)
    sooner = jnp.logical_not(last)
    parts = [y] + [(y + i) % ys for i in range(1, ys)]

    def away(slot):
        return slot != z

    def home(slot):
        return slot == z

    def never(slot):
        return slot < 0

    def near(slot):
        return (slot != z) & (slot // 2 == x)

    def far(slot):
        return (slot != z) & (slot // 2 != x)

    def outer(slot):
        return far(slot) & ((slot == 0) | (slot == zs - 1))

    def inner(slot):
        return far(slot) & (slot != 0) & (slot != zs - 1)

    def is_first(slot):
        return slot == beside

    def is_plain(slot):
        return (slot != z) & (slot != beside)

    def near_plain(slot):
        return near(slot) & (slot != beside)

    def far_plain(slot):
        return far(slot) & (slot != beside)

    def near_first(slot):
        return (slot == beside) & (slot // 2 == x)

    def far_first(slot):
        return (slot == beside) & (slot // 2 != x)

    def slot_at(i):
        outer = jnp.where(i % 2 == 0, zs - 1 - i // 2, i // 2)
        return jnp.where(z < zs // 2, outer, zs - 1 - outer)

    def late_of(c):
        return late_ids[(c - early) * len(halves) : (c - early + 1) * len(halves)]

    queue, done = [], {hop: 0 for hop in range(1, zs - 1)}

    def advance(hop, limit):
        while hop in done and done[hop] < min(limit, len(queue)):
            follow(*queue[done[hop]], hop)
            done[hop] += 1

    def tick():
        for hop in done:
            advance(hop, len(queue) - LAG - (hop - 1) * SKEW)

    def flush():
        while any(place < len(queue) for place in done.values()):
            for hop in done:
                ahead = done.get(hop - 1, len(queue))
                limit = ahead if ahead == len(queue) else ahead - 1
                advance(hop, min(done[hop] + hop, limit))

    def follow(ms, passed, hop):
        @pl.loop(0, zs)
        def _(i):
            slot = slot_at(i)

            @pl.when(passed(slot))
            def _():
                for m in ms:
                    pass_on(slot, m, hop)

    def run(ms, when, passed):
        @pl.loop(0, zs)
        def _(i):
            slot = slot_at(i)

            @pl.when(when(slot))
            def _():
                for m in ms:
                    compute(slot, m)

        if passed is not never:
            queue.append((ms, passed))

    def gather_partner(slot, c_first, c_end, when):
        @pl.when(when(slot))
        def _():
            for c in range(c_first, c_end):
                for part in parts:
                    arrive(slot, part, c)

    steps = list(range(2 * zs - 1))
    share = -(-len(steps) // 7)

    def coef_steps():
        for step in steps[:share]:
            coef_step(step)
        del steps[:share]

    loads[0].wait()
    loads[1].wait()
    make_sent(0)
    meet()

    @pl.when(sooner)
    def _():
        send_y(0)

    make_own(0)

    @pl.when(sooner)
    def _():
        send_x(y, 0)

    for c in range(1, early):
        make_sent(c)

        @pl.when(sooner)
        def _():
            send_y(c)

    pltpu.make_async_copy(attn.at[:, mine, :], attn.at[:, mine, :], attn_sem).wait()
    send_attn(0, two)

    @pl.when(first)
    def _():
        for c in range(early, chunks):
            make_sent(c)
            send_y(c)

    send_attn(two, strips - rest)

    @pl.when(jnp.logical_not(plain))
    def _():
        send_attn(strips - rest, strips)

    for c in range(1, early):
        make_own(c)
    for load in loads[2:]:
        load.wait()

    coef_partial(0)
    for c in range(early):
        @pl.when(sooner)
        def _():
            relay_y(c)
            if c + 1 < early:
                send_x(y, c + 1)

        if c == 0:
            relay_x(y, 0, away)
        coef_partial(1 + c if early > 1 else 1)
    for quarter in range(1 + max(early, 1), quarters):
        coef_partial(quarter)
    coef_steps()
    for part in parts[1:]:
        relay_x(part, 0, away)

    @pl.when(first)
    def _():
        for c in range(early, chunks):
            make_own(c)
            send_x(y, c)

    attn_arrive(0)
    gather_partner(partner, 0, early, away)
    run([0], near, near)
    tick()
    coef_steps()
    for c in range(1, early):
        relay_x(y, c, away)
    coef_steps()
    if two > 1:
        attn_arrive(1)
        run([1], near, near)
        tick()
    coef_steps()
    for c in range(1, early):
        for part in parts[1:]:
            relay_x(part, c, away)
    catch = min(two + 2, strips - 1)
    for other in others:
        gather_partner(other + 1 - core, 0, early, away)
    for k in range(two):
        run([k], far, far)
        tick()
    if rest:
        @pl.when(plain | last)
        def _():
            for c in range(early, chunks):
                make_sent(c)

        @pl.when(plain)
        def _():
            for n in range(rest):
                send_y(early + n)
                send_attn(strips - rest + n, strips - rest + n + 1)

        @pl.when(plain | last)
        def _():
            for c in range(early, chunks):
                make_own(c)

        @pl.when(plain)
        def _():
            for c in range(early, chunks):
                send_x(y, c)

    @pl.when(last)
    def _():
        for c in range(chunks):
            send_y(c)

    def late_near(c, ms):
        @pl.when(plain)
        def _():
            relay_y(c)

        relay_x(y, c, is_plain)
        gather_partner(partner, c, c + 1, is_plain)
        run(ms, near_plain, near)

    def late_far(c):
        for part in parts[1:]:
            relay_x(part, c, is_plain)
        for other in others:
            gather_partner(other + 1 - core, c, c + 1, is_plain)

    for k in range(two, strips):
        n = k - (strips - rest)
        if n >= 0:
            late_near(early + n, late_of(early + n)[:1])
        if n == 1:
            late_far(early)
            run(late_of(early)[:1], far_plain, far)
        if k == two and rest:
            @pl.when(first)
            def _():
                for c in range(early, chunks):
                    relay_y(c)

        attn_arrive(k)
        run([k], away, away)
        tick()
        if rest:
            have = soon_ids[: k - two + 2]
            if k == two:
                gather_partner(partner, early, chunks, is_first)
            run(have if k == two else have[-1:], near_first, never)
            if k == catch:
                for c in range(early, chunks):
                    for part in parts:
                        relay_x(part, c, is_first)
                for other in others:
                    gather_partner(other + 1 - core, early, chunks, is_first)
            if k >= catch:
                run(have if k == catch else have[-1:], far_first, never)
        if k % 2:
            coef_steps()
        if k == two:
            @pl.when(last)
            def _():
                for c in range(chunks):
                    send_x(y, c)
    while steps:
        coef_steps()
    coef_a[2] = coef_a[1]
    coef_partner(True)

    for c in range(chunks):
        relay_x(y, c, home)
    started = len(queue)

    @pl.when(last)
    def _():
        for c in range(chunks // 2):
            relay_y(c)

    if rest:
        run([m for c in range(early, chunks) for m in late_of(c)[1:]], near_plain, near)
        advance(1, started)

    @pl.when(last)
    def _():
        for c in range(chunks // 2, chunks):
            relay_y(c)

    advance(2, started - 1)
    coef_partner(False)
    coef_c[x] = coef_a[2] + coef_b[2]
    for n in range(1, xs):
        coef_x(n, x).start()
    if rest:
        left = list(late_of(early)[1:])
        for c in range(early + 1, chunks):
            late_far(c)
            left += late_of(c)
        run(left, far_plain, outer)
        queue.append((left, inner))
        advance(1, len(queue))
    for n in range(1, xs):
        coef_x(n, (x + n) % xs).wait_recv()
    total = coef_c[0]
    for n in range(1, xs):
        total += coef_c[n]
    coef_c[xs + y] = total
    for i in range(1, ys):
        coef_y(i, y).start()

    for c in range(chunks):
        for part in parts[1:]:
            relay_x(part, c, home)
    flush()

    @pl.when(z % 2 != core)
    def _():
        for c in range(chunks):
            for part in parts:
                arrive(z, part, c)

    width = 2 - strips % 2

    @pl.loop(0, strips, step=width)
    def _(k):
        for n, value in enumerate(product(z, k, 0, chunks, width)):
            own[z, k + n] = value

    for i in range(1, ys):
        coef_y(i, (y + i) % ys).wait_recv()
    total = coef_c[xs]
    for i in range(1, ys):
        total += coef_c[xs + i]
    coef_b[2] = total
    coef_store = pltpu.make_async_copy(coef_b.at[2], coef_out, load_sem.at[0])
    coef_store.start()

    def from_left():
        pltpu.make_async_remote_copy(
            src_ref=z_left.at[z], dst_ref=z_left.at[z],
            send_sem=z_send_sem.at[z], recv_sem=z_sem.at[zs * passing],
            device_id={"dp": dp - ys}, device_id_type=mesh_id,
        ).wait_recv()

    def from_right():
        pltpu.make_async_remote_copy(
            src_ref=z_right.at[z], dst_ref=z_right.at[z],
            send_sem=z_send_sem.at[z], recv_sem=z_sem.at[zs * passing + 1],
            device_id={"dp": dp + ys}, device_id_type=mesh_id,
        ).wait_recv()

    low = z < zs // 2
    high = jnp.logical_not(low)

    @pl.when(low & (z > 0))
    def _():
        from_left()

        @pl.loop(0, strips)
        def _(k):
            own[z, k] += z_left[z, k].astype(jnp.float32)

    @pl.when(high & (z < zs - 1))
    def _():
        from_right()

        @pl.loop(0, strips)
        def _(k):
            own[z, k] += z_right[z, k].astype(jnp.float32)

    @pl.when(low)
    def _():
        from_right()

    @pl.when(high)
    def _():
        from_left()

    for c in range(chunks):
        at = lane_rows(c)

        @pl.when(low)
        def _():
            for k in range(strips):
                lanes = slice(k * LANES, (k + 1) * LANES)
                result[at, lanes] = own[z, k, at, :] + z_right[z, k, at, :].astype(jnp.float32)

        @pl.when(high)
        def _():
            for k in range(strips):
                lanes = slice(k * LANES, (k + 1) * LANES)
                result[at, lanes] = own[z, k, at, :] + z_left[z, k, at, :].astype(jnp.float32)

        pltpu.make_async_copy(result.at[at, :], proj_out.at[at, :], attn_sem).start()

    @pl.loop(0, zs)
    def _(slot):
        @pl.when(slot != z)
        def _():
            pltpu.make_async_remote_copy(
                src_ref=z_send.at[slot], dst_ref=z_left.at[slot],
                send_sem=z_send_sem.at[slot], recv_sem=z_sem.at[0],
                device_id={"dp": z * ys + (y + 1) % ys}, device_id_type=mesh_id,
            ).wait_send()

    def sent(ref, sem):
        pltpu.make_async_remote_copy(
            src_ref=ref, dst_ref=ref, send_sem=sem, recv_sem=z_sem.at[0],
            device_id={"tensor": partner}, device_id_type=mesh_id,
        ).wait_send()

    for i in range(1, ys):
        sent(g_send.at[i - 1], gy_sem.at[i - 1])
        sent(attn.at[:, mine, :], a_sem.at[i - 1])
    for n in range(xs):
        sent(gathered.at[n * 2 + core], p_sem.at[n])
    for n in range(1, xs):
        sent(gathered.at[tensor], x_sem.at[n - 1])

    @pl.when(z < zs - 1)
    def _():
        coef_hop(0, {"dp": dp + ys}).wait_send()

    @pl.when(z > 0)
    def _():
        coef_hop(1, {"dp": dp - ys}).wait_send()

    coef_hop(2, {"tensor": partner}).wait_send()
    for n in range(1, xs):
        coef_x(n, x).wait_send()
    for i in range(1, ys):
        coef_y(i, y).wait_send()
    coef_store.wait()
    pltpu.make_async_copy(result, proj_out, attn_sem).wait()


def settle(coef, proj, coef_out, proj_out):
    coef_out[...] = coef[: coef_out.shape[0], : coef_out.shape[1]]
    proj_out[...] = proj[...]


def local(dp_size, tensor_size, layer_outs, avg_grads, attn_mixed, dwa_coefs):
    depth, tokens, features = avg_grads.shape
    rows = features * tensor_size // dp_size
    cols = attn_mixed.shape[1]
    ys, zs, xs = dp_size // tensor_size, tensor_size, tensor_size // 2
    strips, chunks = cols // LANES, rows // LANES
    bf16, f32 = jnp.bfloat16, jnp.float32
    dma = pltpu.SemaphoreType.DMA
    any_space = pl.BlockSpec(memory_space=pl.ANY)
    coef, proj = pl.pallas_call(
        functools.partial(kernel, dp_size, tensor_size),
        out_shape=(
            jax.ShapeDtypeStruct((8, LANES), f32),
            jax.ShapeDtypeStruct((rows, cols), f32),
        ),
        in_specs=[any_space, any_space, any_space, pl.BlockSpec(memory_space=pltpu.SMEM)],
        out_specs=(any_space, any_space),
        scratch_shapes=[
            pltpu.VMEM(layer_outs.shape, bf16),
            pltpu.VMEM(avg_grads.shape, bf16),
            pltpu.VMEM((strips, ys * tokens, LANES), bf16),
            pltpu.VMEM((zs, ys, rows, tokens), bf16),
            pltpu.VMEM((ys - 1, rows, tokens), bf16),
            pltpu.VMEM((zs, strips, rows, LANES), f32),
            pltpu.VMEM((zs, strips, rows, LANES), bf16),
            pltpu.VMEM((zs, strips, rows, LANES), bf16),
            pltpu.VMEM((zs, strips, rows, LANES), bf16),
            pltpu.VMEM((depth * (depth + 1), 8, LANES), f32),
            pltpu.VMEM((3, 8, LANES), f32),
            pltpu.VMEM((3, 8, LANES), f32),
            pltpu.VMEM((xs + ys, 8, LANES), f32),
            pltpu.VMEM((rows, cols), f32),
            dma((2 * depth + 1,)),
            dma,
            dma((ys - 1,)),
            dma((xs,)),
            dma((max(xs - 1, 1),)),
            dma((tensor_size, ys, chunks)),
            dma((ys - 1,)),
            dma((ys - 1, strips)),
            dma((zs,)),
            dma((zs * (strips + chunks) + 2,)),
            dma((3,)),
            dma((3,)),
            dma((xs + ys,)),
            dma((xs + ys,)),
        ],
        compiler_params=pltpu.CompilerParams(
            collective_id=0, has_side_effects=True, vmem_limit_bytes=67000000
        ),
    )(layer_outs, avg_grads, attn_mixed, dwa_coefs)
    half = rows // 2
    return pl.pallas_call(
        settle,
        grid=(2,),
        out_shape=(
            jax.ShapeDtypeStruct(dwa_coefs.shape, f32),
            jax.ShapeDtypeStruct((rows, cols), f32),
        ),
        in_specs=[
            pl.BlockSpec((8, LANES), lambda i: (0, 0)),
            pl.BlockSpec((half, cols), lambda i: (i, 0)),
        ],
        out_specs=(
            pl.BlockSpec(dwa_coefs.shape, lambda i: (0, 0)),
            pl.BlockSpec((half, cols), lambda i: (i, 0)),
        ),
    )(coef, proj)


def solution(mesh):
    sizes = (mesh.shape["dp"], mesh.shape["tensor"])
    in_specs = (P(None, "dp", "tensor"), P(None, "dp", "tensor"), P("dp", "tensor"), P())
    out_specs = (P(), P("dp", "tensor"))
    return jax.shard_map(
        functools.partial(local, *sizes), mesh=mesh, in_specs=in_specs, out_specs=out_specs, check_vma=False
    )
```
